256 devices in a mesh: frag: 2 (over z), grid: 128 (over y, x, core).
Axes of the slice: x: 8, y: 8, z: 2, core: 2. Of those that a mesh axis runs over, the one named last changes fastest.
The devices are a block of a 8x8x16 slice.
Arguments:
- psi: float32 [131072, 640], P(('frag', 'grid')), parts along dimension 0
- order: int32 [10], P('frag'), parts along dimension 0, may hold values from 0 to 4, each once
Outputs:
- orthonormal: float32 [131072, 640], P(('frag', 'grid')), parts along dimension 0
The draws below stay inside these ranges and needn't reach their ends.
There are 2 independent parts, one for each index of `frag`. The reference program is written for one: setup_inputs(seed, part) draws one part's arguments, and reference() takes and returns one part's arrays. A program takes and returns all parts, laid end to end along the dimension named above; each array names one. Nothing has to cross between parts.
All inputs are finite; a program needn't handle non-finite values.
Results may differ from the reference program's by a relative error of at most 0.00012.
Values sent between devices are 32-bit elements; how exact they have to be, the bound alone decides.
No kernel may reach another device: no remote copies, remote signals or barrier semaphores. Data moves between devices by JAX's collectives and lax.ppermute only.
A program may use at most 64 MiB of HBM per device.

```python
import jax
import jax.numpy as jnp
from jax import lax

BLOCK = 128
NBLK = 5
BANDS = 640
POINTS = 65536


def draw_psi(key, part):
    own = jax.random.normal(jax.random.fold_in(key, 11), (POINTS, BANDS), jnp.float32)
    shared = jax.random.normal(jax.random.fold_in(key, 12), (POINTS, BLOCK), jnp.float32)
    mixed = own + 0.8 * jnp.tile(shared, (1, NBLK))
    return mixed.astype(jnp.float32)


def setup_inputs(seed: int = 0, part: int = 0) -> dict:
    streams_of = jax.random.split(jax.random.key(seed), 3)
    part_splits = jax.random.split(jax.random.fold_in(streams_of[2], part), 3)
    psi = draw_psi(jax.random.fold_in(jax.random.fold_in(streams_of[2], part), 71), part)
    order = jax.random.permutation(part_splits[1], NBLK).astype(jnp.int32)
    return {"psi": psi, "order": order}


def contract(left, right):
    return lax.dot_general(left.astype(jnp.float32), right.astype(jnp.float32), (((0,), (0,)), ((), ())), precision=lax.Precision.HIGHEST, preferred_element_type=jnp.float32)

def matmul(left, right):
    return jnp.dot(left.astype(jnp.float32), right.astype(jnp.float32), precision=lax.Precision.HIGHEST, preferred_element_type=jnp.float32)

def reference(psi, order):
    scale = jnp.float32(1.0 / POINTS)
    result = jnp.zeros_like(psi)
    done = []
    for step in range(NBLK):
        start = (order[step] * BLOCK).astype(jnp.int32)
        block = lax.dynamic_slice_in_dim(psi, start, BLOCK, 1)
        if step > 0:
            prev = jnp.concatenate(done, axis=1)
            coeff = contract(prev, block) * scale
            block = block - matmul(prev, coeff)
        gram = contract(block, block) * scale
        lower = jnp.linalg.cholesky(gram)
        inverse = lax.linalg.triangular_solve(lower, jnp.eye(BLOCK, dtype=gram.dtype), left_side=True, lower=True)
        basis = matmul(block, inverse.T)
        done.append(basis)
        result = lax.dynamic_update_slice(result, basis, (jnp.int32(0), start))
    return result
```

```python
import jax
import jax.numpy as jnp
from jax import lax
from jax.experimental import pallas as pl
from jax.experimental.pallas import tpu as pltpu
from jax.sharding import PartitionSpec as P

BLOCK = 128
NBLK = 5
PANEL = 16
PAIRS = [(i, j) for i in range(NBLK) for j in range(i, NBLK)]
SLOTS = 16
HIGHEST = lax.Precision.HIGHEST


def dot(left, right, contract):
    return lax.dot_general(
        left, right, (contract, ((), ())), precision=HIGHEST, preferred_element_type=jnp.float32
    )


def cols(ref, block):
    return ref[:, pl.ds(pl.multiple_of(block * BLOCK, BLOCK), BLOCK)]


def gram_kernel(scale, order_ref, psi_ref, out_ref, perm_ref):
    for i in range(NBLK):
        perm_ref[:, i * BLOCK:(i + 1) * BLOCK] = cols(psi_ref, order_ref[i])
    slot = 0
    for i in range(NBLK):
        row = dot(perm_ref[:, i * BLOCK:(i + 1) * BLOCK], perm_ref[:, i * BLOCK:], ((0,), (0,))) * scale
        for j in range(NBLK - i):
            out_ref[slot] = row[:, j * BLOCK:(j + 1) * BLOCK]
            slot += 1
    for extra in range(slot, SLOTS):
        out_ref[extra] = jnp.zeros((BLOCK, BLOCK), jnp.float32)


def factor_block(work_ref):
    row = lax.broadcasted_iota(jnp.int32, (PANEL, BLOCK), 0)
    for p in range(BLOCK // PANEL):
        r0 = p * PANEL
        part_a = work_ref[r0:r0 + PANEL, :BLOCK]
        part_e = work_ref[r0:r0 + PANEL, BLOCK:]
        columns = [
            jnp.broadcast_to(part_a[:, r0 + m:r0 + m + 1], (PANEL, BLOCK)) for m in range(PANEL)
        ]
        diag = jnp.ones((PANEL, BLOCK), jnp.float32)
        for k in range(PANEL):
            column = columns[k]
            pivot = column[k:k + 1, :]
            diag = jnp.where(row == k, pivot, diag)
            if k == PANEL - 1:
                break
            factor = jnp.where(row > k, column * (1.0 / pivot), 0.0)
            for m in range(k + 1, PANEL):
                columns[m] = columns[m] - factor * column[m:m + 1, :]
            part_a = part_a - factor * part_a[k:k + 1, :]
            part_e = part_e - factor * part_e[k:k + 1, :]
        norm = lax.rsqrt(diag)
        part_a = part_a * norm
        part_e = part_e * norm
        work_ref[r0:r0 + PANEL, BLOCK:] = part_e
        low = r0 + PANEL
        if low < BLOCK:
            both = jnp.concatenate([part_a, part_e], axis=1)
            update = dot(part_a, both, ((0,), (0,)))
            work_ref[low:, :] = work_ref[low:, :] - update[low:, :]
    return work_ref[:, BLOCK:]


def factor_kernel(core_ref, mine_ref, other_ref, out_ref, grid_ref, work_ref):
    core = core_ref[0]
    half = SLOTS // 2
    for slot, (i, j) in enumerate(PAIRS):
        own = (core == slot // half)
        value = jnp.where(own, mine_ref[slot % half], other_ref[slot % half])
        grid_ref[i, :, j * BLOCK:(j + 1) * BLOCK] = value
    for i in range(1, NBLK):
        grid_ref[i, :, :i * BLOCK] = jnp.zeros((BLOCK, i * BLOCK), jnp.float32)
    eye = (
        lax.broadcasted_iota(jnp.int32, (BLOCK, BLOCK), 0)
        == lax.broadcasted_iota(jnp.int32, (BLOCK, BLOCK), 1)
    ).astype(jnp.float32)
    for k in range(NBLK):
        here = slice(k * BLOCK, (k + 1) * BLOCK)
        after = slice((k + 1) * BLOCK, NBLK * BLOCK)
        work_ref[:, :BLOCK] = grid_ref[k, :, here]
        work_ref[:, BLOCK:] = eye
        inverse = factor_block(work_ref)
        grid_ref[k, :, here] = inverse
        if k + 1 < NBLK:
            right = dot(inverse, grid_ref[k, :, after], ((1,), (0,)))
            grid_ref[k, :, after] = right
        if k > 0:
            grid_ref[k, :, :k * BLOCK] = dot(inverse, grid_ref[k, :, :k * BLOCK], ((1,), (0,)))
        for i in range(k + 1, NBLK):
            lead = grid_ref[k, :, i * BLOCK:(i + 1) * BLOCK]
            grid_ref[i, :, i * BLOCK:] = grid_ref[i, :, i * BLOCK:] - dot(
                lead, grid_ref[k, :, i * BLOCK:], ((0,), (0,))
            )
            grid_ref[i, :, :(k + 1) * BLOCK] = grid_ref[i, :, :(k + 1) * BLOCK] - dot(
                lead, grid_ref[k, :, :(k + 1) * BLOCK], ((0,), (0,))
            )
    out_ref[...] = jnp.zeros(out_ref.shape, jnp.float32)
    for i in range(NBLK):
        for j in range(i + 1):
            out_ref[j * BLOCK:(j + 1) * BLOCK, i * BLOCK:(i + 1) * BLOCK] = (
                grid_ref[i, :, j * BLOCK:(j + 1) * BLOCK].T
            )


def apply_kernel(order_ref, psi_ref, inv_ref, out_ref, perm_ref):
    for i in range(NBLK):
        perm_ref[:, i * BLOCK:(i + 1) * BLOCK] = cols(psi_ref, order_ref[i])
    for first in range(0, NBLK, 2):
        last = min(first + 2, NBLK)
        value = dot(
            perm_ref[:, :last * BLOCK],
            inv_ref[:last * BLOCK, first * BLOCK:last * BLOCK],
            ((1,), (0,)),
        )
        for b in range(first, last):
            start = pl.multiple_of(order_ref[b] * BLOCK, BLOCK)
            out_ref[:, pl.ds(start, BLOCK)] = value[:, (b - first) * BLOCK:(b - first + 1) * BLOCK]


def vmem():
    return pl.BlockSpec(memory_space=pltpu.VMEM)


def smem():
    return pl.BlockSpec(memory_space=pltpu.SMEM)


def local(psi, order):
    rows, bands = psi.shape
    size = lax.axis_size("grid")
    chips = size // 2
    scale = 1.0 / (rows * size)
    index = lax.axis_index("grid")
    core = index % 2
    pairs = [(d, d ^ 1) for d in range(size)]
    groups = [list(range(c, size, 2)) for c in range(2)]
    half = SLOTS // 2
    chunk = half * BLOCK // chips

    gram = pl.pallas_call(
        lambda *refs: gram_kernel(scale, *refs),
        out_shape=jax.ShapeDtypeStruct((SLOTS, BLOCK, BLOCK), jnp.float32),
        in_specs=[smem(), vmem()],
        out_specs=vmem(),
        scratch_shapes=[pltpu.VMEM((rows, bands), jnp.float32)],
        name="gram",
    )(order, psi)

    gram = gram.reshape(2, half, BLOCK, BLOCK)
    keep = lax.dynamic_index_in_dim(gram, core, 0, keepdims=False)
    send = lax.dynamic_index_in_dim(gram, 1 - core, 0, keepdims=False)
    both = keep + lax.ppermute(send, "grid", pairs)
    parts = lax.all_to_all(
        both.reshape(chips, chunk, BLOCK), "grid", 0, 0, axis_index_groups=groups, tiled=True
    )
    total = jnp.sum(parts, axis=0)
    mine = lax.all_to_all(
        jnp.broadcast_to(total[None], parts.shape), "grid", 0, 0, axis_index_groups=groups, tiled=True
    ).reshape(half, BLOCK, BLOCK)
    other = lax.ppermute(mine, "grid", pairs)

    inverse = pl.pallas_call(
        factor_kernel,
        out_shape=jax.ShapeDtypeStruct((bands, bands), jnp.float32),
        in_specs=[smem(), vmem(), vmem()],
        out_specs=vmem(),
        scratch_shapes=[
            pltpu.VMEM((NBLK, BLOCK, bands), jnp.float32),
            pltpu.VMEM((BLOCK, 2 * BLOCK), jnp.float32),
        ],
        name="factor",
    )(core.astype(jnp.int32).reshape(1), mine, other)

    return pl.pallas_call(
        apply_kernel,
        out_shape=jax.ShapeDtypeStruct((rows, bands), jnp.float32),
        in_specs=[smem(), vmem(), vmem()],
        out_specs=vmem(),
        scratch_shapes=[pltpu.VMEM((rows, bands), jnp.float32)],
        name="apply",
    )(order, psi, inverse)


def solution(mesh):
    in_specs = (P(("frag", "grid"), None), P("frag"))
    out_specs = P(("frag", "grid"), None)
    return jax.shard_map(local, mesh=mesh, in_specs=in_specs, out_specs=out_specs, check_vma=False)
```

```python
import jax
import jax.numpy as jnp
from jax import lax
from jax.experimental import pallas as pl
from jax.experimental.pallas import tpu as pltpu
from jax.sharding import PartitionSpec as P

BLOCK = 128
NBLK = 5
PANEL = 32
SUB = 8
PAIRS = [(i, j) for i in range(NBLK) for j in range(i, NBLK)]
SLOT = {pair: slot for slot, pair in enumerate(PAIRS)}
SLOTS = 16
HIGHEST = lax.Precision.HIGHEST


def dot(left, right):
    return lax.dot_general(
        left, right, (((1,), (0,)), ((), ())), precision=HIGHEST, preferred_element_type=jnp.float32
    )


def dot_tn(left, right):
    return lax.dot_general(
        left, right, (((0,), (0,)), ((), ())), precision=HIGHEST, preferred_element_type=jnp.float32
    )


def dot_nt(left, right):
    return lax.dot_general(
        left, right, (((1,), (1,)), ((), ())), precision=HIGHEST, preferred_element_type=jnp.float32
    )


def span(first, last):
    return slice(first * BLOCK, last * BLOCK)


def block_copies(order_ref, far_ref, near_ref, sems, outward=False):
    copies = []
    for b in range(NBLK):
        start = pl.multiple_of(order_ref[b] * BLOCK, BLOCK)
        far = far_ref.at[:, pl.ds(start, BLOCK)]
        near = near_ref.at[:, span(b, b + 1)]
        copies.append(
            pltpu.make_async_copy(near, far, sems.at[b])
            if outward
            else pltpu.make_async_copy(far, near, sems.at[b])
        )
    return copies


def gram_kernel(scale, order_ref, psi_ref, out_ref, x_ref, sems):
    loads = block_copies(order_ref, psi_ref, x_ref, sems)
    for load in loads:
        load.start()
    for load in loads:
        load.wait()
    for i in range(NBLK):
        row = dot_tn(x_ref[:, span(i, i + 1)], x_ref[:, i * BLOCK:]) * scale
        for j in range(i, NBLK):
            out_ref[SLOT[i, j]] = row[:, span(j - i, j - i + 1)]
    for extra in range(len(PAIRS), SLOTS):
        out_ref[extra] = jnp.zeros((BLOCK, BLOCK), jnp.float32)


def eliminate(work_ref, col_ref, between):
    lane = lax.broadcasted_iota(jnp.int32, (SUB, BLOCK), 1)
    row = lax.broadcasted_iota(jnp.int32, (SUB, BLOCK), 0)
    pieces = PANEL // SUB
    for p in range(BLOCK // PANEL):
        r0 = p * PANEL
        low = r0 + PANEL
        for m in range(PANEL):
            top = m // SUB * SUB
            col_ref[m, top:, :] = jnp.broadcast_to(
                work_ref[r0 + top:low, r0 + m:r0 + m + 1], (PANEL - top, BLOCK)
            )
        inside = (lane >= r0) & (lane < low)
        part = []
        for q in range(pieces):
            unit = (lane == row + (r0 + q * SUB)).astype(jnp.float32)
            part.append(jnp.where(inside, unit, work_ref[r0 + q * SUB:r0 + (q + 1) * SUB, :]))
        column = {
            (m, q): col_ref[m, q * SUB:(q + 1) * SUB, :]
            for m in range(PANEL)
            for q in range(m // SUB, pieces)
        }
        diag = [jnp.ones((SUB, BLOCK), jnp.float32)] * pieces
        for k in range(PANEL):
            kq, ks = divmod(k, SUB)
            pivot = column[k, kq][ks:ks + 1, :]
            inverse = 1.0 / pivot
            diag[kq] = jnp.where(row == ks, pivot, diag[kq])
            factor = {q: column[k, q] * inverse for q in range(kq, pieces)}
            for m in range(k + 1, PANEL):
                mq, ms = divmod(m, SUB)
                entry = column[k, mq][ms:ms + 1, :]
                for q in range(mq, pieces):
                    column[m, q] = column[m, q] - factor[q] * entry
            lead = part[kq][ks:ks + 1, :]
            part[kq] = part[kq] - jnp.where(row > ks, factor[kq], 0.0) * lead
            for q in range(kq + 1, pieces):
                part[q] = part[q] - factor[q] * lead
        whole = jnp.concatenate([part[q] * lax.rsqrt(diag[q]) for q in range(pieces)], axis=0)
        work_ref[r0:low, :] = whole
        if low < BLOCK:
            update = dot(whole.T[low:, :], whole)
            rest = lax.broadcasted_iota(jnp.int32, (BLOCK - low, BLOCK), 1)
            kept = jnp.where((rest >= r0) & (rest < low), 0.0, work_ref[low:, :])
            work_ref[low:, :] = kept - update
        between()


def finish_kernel(
    core_ref, order_ref, mine_ref, other_ref, psi_ref, out_ref,
    a_ref, inv_ref, pair_ref, x_ref, q_ref, work_ref, col_ref, in_sems, out_sems,
):
    loads = block_copies(order_ref, psi_ref, x_ref, in_sems)
    stores = block_copies(order_ref, out_ref, q_ref, out_sems, outward=True)
    for load in loads:
        load.start()
    core = core_ref[0]
    half = SLOTS // 2
    for slot, (i, j) in enumerate(PAIRS):
        own = core == slot // half
        a_ref[span(i, i + 1), span(j, j + 1)] = jnp.where(
            own, mine_ref[slot % half], other_ref[slot % half]
        )
    lower = (
        lax.broadcasted_iota(jnp.int32, (BLOCK, BLOCK), 0)
        >= lax.broadcasted_iota(jnp.int32, (BLOCK, BLOCK), 1)
    )
    rows = x_ref.shape[0]
    tiles = [slice(r, r + BLOCK) for r in range(0, rows, BLOCK)]
    soon, whenever = [], []

    def a(i, j, wide=1):
        return a_ref[span(i, i + 1), span(j, j + wide)]

    def solve(k, j, wide=1):
        a_ref[span(k, k + 1), span(j, j + wide)] = dot(inv_ref[k], a(k, j, wide))

    def downdate(i, j, first, last, wide=1):
        ks = span(first, last)
        a_ref[span(i, i + 1), span(j, j + wide)] = a(i, j, wide) - dot_tn(
            a_ref[ks, span(i, i + 1)], a_ref[ks, span(j, j + wide)]
        )

    def couple(k):
        pair_ref[k, BLOCK:, :BLOCK] = dot_tn(a(k, k + 1), inv_ref[k])

    def pair(k):
        pair_ref[k, :BLOCK, :BLOCK] = inv_ref[k]
        pair_ref[k, BLOCK:, BLOCK:] = inv_ref[k + 1]
        pair_ref[k, :BLOCK, BLOCK:] = jnp.zeros((BLOCK, BLOCK), jnp.float32)
        pair_ref[k, BLOCK:, :BLOCK] = -dot(inv_ref[k + 1], pair_ref[k, BLOCK:, :BLOCK])

    def finish(k, wide, tile):
        factor = pair_ref[k] if wide == 2 else inv_ref[k]
        q_ref[tile, span(k, k + wide)] = dot_nt(x_ref[tile, span(k, k + wide)], factor)

    def project(first, last, tile):
        x_ref[tile, last * BLOCK:] = x_ref[tile, last * BLOCK:] - dot(
            q_ref[tile, span(first, last)], a_ref[span(first, last), last * BLOCK:]
        )

    def send(first, last):
        for b in range(first, last):
            stores[b].start()

    def after(k):
        if k + 1 == NBLK:
            return
        solve(k, k + 1)
        downdate(k + 1, k + 1, k, k + 1)
        first = k // 2 * 2
        if k % 2 == 0:
            soon.append(lambda: couple(k))
            if k + 2 < NBLK:
                soon.append(lambda: solve(k, k + 2))
                soon.append(lambda: downdate(k + 1, k + 2, k, k + 1))
                soon.append(lambda: downdate(k + 2, k + 2, k, k + 1))
            if k + 3 < NBLK:
                soon.append(lambda: solve(k, k + 3, NBLK - k - 3))
                soon.append(lambda: downdate(k + 1, k + 3, k, k + 1, NBLK - k - 3))
        else:
            if k + 2 < NBLK:
                soon.append(lambda: solve(k, k + 2, NBLK - k - 2))
                soon.append(lambda: downdate(k + 1, k + 2, first, k + 1, NBLK - k - 2))
                for i in range(k + 2, NBLK):
                    soon.append(lambda i=i: downdate(i, i, first, k + 1, NBLK - i))
            whenever.append(lambda: pair(first))
            for tile in tiles:
                whenever.append(lambda tile=tile: finish(first, 2, tile))
            whenever.append(lambda: send(first, k + 1))
            for tile in tiles:
                whenever.append(lambda tile=tile: project(first, k + 1, tile))

    def run(queue, count):
        for _ in range(min(count, len(queue))):
            queue.pop(0)()

    panels = BLOCK // PANEL
    for k in range(NBLK):
        work_ref[...] = a(k, k)
        state = {"left": panels}

        def between():
            run(soon, -(-len(soon) // max(state["left"] - 1, 1)))
            more = panels if k % 2 == 0 and k + 1 < NBLK else 0
            turns = state["left"] + more
            run(whenever, -(-len(whenever) // turns))
            state["left"] -= 1

        eliminate(work_ref, col_ref, between)
        run(soon, len(soon))
        inv_ref[k] = jnp.where(lower, work_ref[...], 0.0)
        if k == 1:
            for load in loads:
                load.wait()
        after(k)
    run(whenever, len(whenever))
    last = NBLK - 1
    for tile in tiles:
        finish(last, 1, tile)
    send(last, NBLK)
    for store in stores:
        store.wait()


def vmem():
    return pl.BlockSpec(memory_space=pltpu.VMEM)


def smem():
    return pl.BlockSpec(memory_space=pltpu.SMEM)


def anywhere():
    return pl.BlockSpec(memory_space=pl.ANY)


def finish_scratch(rows):
    bands = NBLK * BLOCK
    return [
        pltpu.VMEM((bands, bands), jnp.float32),
        pltpu.VMEM((NBLK, BLOCK, BLOCK), jnp.float32),
        pltpu.VMEM((NBLK, 2 * BLOCK, 2 * BLOCK), jnp.float32),
        pltpu.VMEM((rows, bands), jnp.float32),
        pltpu.VMEM((rows, bands), jnp.float32),
        pltpu.VMEM((BLOCK, BLOCK), jnp.float32),
        pltpu.VMEM((PANEL, PANEL, BLOCK), jnp.float32),
        pltpu.SemaphoreType.DMA((NBLK,)),
        pltpu.SemaphoreType.DMA((NBLK,)),
    ]


def local(psi, order):
    rows, bands = psi.shape
    size = lax.axis_size("grid")
    chips = size // 2
    scale = 1.0 / (rows * size)
    core = lax.axis_index("grid") % 2
    pairs = [(d, d ^ 1) for d in range(size)]
    groups = [list(range(c, size, 2)) for c in range(2)]
    half = SLOTS // 2
    chunk = half * BLOCK // chips

    gram = pl.pallas_call(
        lambda *refs: gram_kernel(scale, *refs),
        out_shape=jax.ShapeDtypeStruct((SLOTS, BLOCK, BLOCK), jnp.float32),
        in_specs=[smem(), anywhere()],
        out_specs=vmem(),
        scratch_shapes=[
            pltpu.VMEM((rows, bands), jnp.float32),
            pltpu.SemaphoreType.DMA((NBLK,)),
        ],
        name="gram",
    )(order, psi)

    gram = gram.reshape(2, half, BLOCK, BLOCK)
    keep = lax.dynamic_index_in_dim(gram, core, 0, keepdims=False)
    send = lax.dynamic_index_in_dim(gram, 1 - core, 0, keepdims=False)
    both = keep + lax.ppermute(send, "grid", pairs)
    parts = lax.all_to_all(
        both.reshape(chips, chunk, BLOCK), "grid", 0, 0, axis_index_groups=groups, tiled=True
    )
    total = jnp.sum(parts, axis=0)
    mine = lax.all_to_all(
        jnp.broadcast_to(total[None], parts.shape), "grid", 0, 0, axis_index_groups=groups, tiled=True
    ).reshape(half, BLOCK, BLOCK)
    other = lax.ppermute(mine, "grid", pairs)

    return pl.pallas_call(
        finish_kernel,
        out_shape=jax.ShapeDtypeStruct((rows, bands), jnp.float32),
        in_specs=[smem(), smem(), vmem(), vmem(), anywhere()],
        out_specs=anywhere(),
        scratch_shapes=finish_scratch(rows),
        name="finish",
    )(core.astype(jnp.int32).reshape(1), order, mine, other, psi)


def solution(mesh):
    in_specs = (P(("frag", "grid"), None), P("frag"))
    out_specs = P(("frag", "grid"), None)
    return jax.shard_map(local, mesh=mesh, in_specs=in_specs, out_specs=out_specs, check_vma=False)
```

```python
import jax
import jax.numpy as jnp
from jax import lax
from jax.experimental import pallas as pl
from jax.experimental.pallas import tpu as pltpu
from jax.sharding import PartitionSpec as P

BLOCK = 128
NBLK = 5
PANEL = 32
SUB = 8
PAIRS = [(i, j) for i in range(NBLK) for j in range(i, NBLK)]
SLOT = {pair: slot for slot, pair in enumerate(PAIRS)}
SLOTS = 16
HIGHEST = lax.Precision.HIGHEST


def dot(left, right):
    return lax.dot_general(
        left, right, (((1,), (0,)), ((), ())), precision=HIGHEST, preferred_element_type=jnp.float32
    )


def dot_tn(left, right):
    return lax.dot_general(
        left, right, (((0,), (0,)), ((), ())), precision=HIGHEST, preferred_element_type=jnp.float32
    )


def dot_nt(left, right):
    return lax.dot_general(
        left, right, (((1,), (1,)), ((), ())), precision=HIGHEST, preferred_element_type=jnp.float32
    )


def span(first, last):
    return slice(first * BLOCK, last * BLOCK)


def block_copies(order_ref, far_ref, near_ref, sems, outward=False):
    copies = []
    for b in range(NBLK):
        start = pl.multiple_of(order_ref[b] * BLOCK, BLOCK)
        far = far_ref.at[:, pl.ds(start, BLOCK)]
        near = near_ref.at[:, span(b, b + 1)]
        copies.append(
            pltpu.make_async_copy(near, far, sems.at[b])
            if outward
            else pltpu.make_async_copy(far, near, sems.at[b])
        )
    return copies


def gram_kernel(scale, order_ref, psi_ref, out_ref, x_ref):
    for i in range(NBLK):
        start = pl.multiple_of(order_ref[i] * BLOCK, BLOCK)
        x_ref[:, span(i, i + 1)] = psi_ref[:, pl.ds(start, BLOCK)]
    for i in range(NBLK):
        row = dot_tn(x_ref[:, span(i, i + 1)], x_ref[:, i * BLOCK:]) * scale
        for j in range(i, NBLK):
            out_ref[SLOT[i, j]] = row[:, span(j - i, j - i + 1)]
    for extra in range(len(PAIRS), SLOTS):
        out_ref[extra] = jnp.zeros((BLOCK, BLOCK), jnp.float32)


def eliminate(work_ref, col_ref, between):
    lane = lax.broadcasted_iota(jnp.int32, (SUB, BLOCK), 1)
    row = lax.broadcasted_iota(jnp.int32, (SUB, BLOCK), 0)
    pieces = PANEL // SUB
    for p in range(BLOCK // PANEL):
        r0 = p * PANEL
        low = r0 + PANEL
        for m in range(PANEL):
            top = m // SUB * SUB
            col_ref[m, top:, :] = jnp.broadcast_to(
                work_ref[r0 + top:low, r0 + m:r0 + m + 1], (PANEL - top, BLOCK)
            )
        inside = (lane >= r0) & (lane < low)
        part = []
        for q in range(pieces):
            unit = (lane == row + (r0 + q * SUB)).astype(jnp.float32)
            part.append(jnp.where(inside, unit, work_ref[r0 + q * SUB:r0 + (q + 1) * SUB, :]))
        column = {
            (m, q): col_ref[m, q * SUB:(q + 1) * SUB, :]
            for m in range(PANEL)
            for q in range(m // SUB, pieces)
        }
        diag = [jnp.ones((SUB, BLOCK), jnp.float32)] * pieces
        for k in range(PANEL):
            kq, ks = divmod(k, SUB)
            pivot = column[k, kq][ks:ks + 1, :]
            inverse = 1.0 / pivot
            diag[kq] = jnp.where(row == ks, pivot, diag[kq])
            factor = {q: column[k, q] * inverse for q in range(kq, pieces)}
            for m in range(k + 1, PANEL):
                mq, ms = divmod(m, SUB)
                entry = column[k, mq][ms:ms + 1, :]
                for q in range(mq, pieces):
                    column[m, q] = column[m, q] - factor[q] * entry
            lead = part[kq][ks:ks + 1, :]
            part[kq] = part[kq] - jnp.where(row > ks, factor[kq], 0.0) * lead
            for q in range(kq + 1, pieces):
                part[q] = part[q] - factor[q] * lead
        whole = jnp.concatenate([part[q] * lax.rsqrt(diag[q]) for q in range(pieces)], axis=0)
        work_ref[r0:low, :] = whole
        if low < BLOCK:
            update = dot(whole.T[low:, :], whole)
            rest = lax.broadcasted_iota(jnp.int32, (BLOCK - low, BLOCK), 1)
            kept = jnp.where((rest >= r0) & (rest < low), 0.0, work_ref[low:, :])
            work_ref[low:, :] = kept - update
        between()


def finish_kernel(
    core_ref, order_ref, mine_ref, other_ref, psi_ref, out_ref,
    a_ref, inv_ref, pair_ref, x_ref, q_ref, work_ref, col_ref, in_sems, out_sems,
):
    loads = block_copies(order_ref, psi_ref, x_ref, in_sems)
    stores = block_copies(order_ref, out_ref, q_ref, out_sems, outward=True)
    for load in loads:
        load.start()
    core = core_ref[0]
    half = SLOTS // 2
    for slot, (i, j) in enumerate(PAIRS):
        own = core == slot // half
        a_ref[span(i, i + 1), span(j, j + 1)] = jnp.where(
            own, mine_ref[slot % half], other_ref[slot % half]
        )
    lower = (
        lax.broadcasted_iota(jnp.int32, (BLOCK, BLOCK), 0)
        >= lax.broadcasted_iota(jnp.int32, (BLOCK, BLOCK), 1)
    )
    rows = x_ref.shape[0]
    tiles = [slice(r, r + BLOCK) for r in range(0, rows, BLOCK)]
    soon, whenever = [], []

    def a(i, j, wide=1):
        return a_ref[span(i, i + 1), span(j, j + wide)]

    def solve(k, j, wide=1):
        a_ref[span(k, k + 1), span(j, j + wide)] = dot(inv_ref[k], a(k, j, wide))

    def downdate(i, j, first, last, wide=1):
        ks = span(first, last)
        a_ref[span(i, i + 1), span(j, j + wide)] = a(i, j, wide) - dot_tn(
            a_ref[ks, span(i, i + 1)], a_ref[ks, span(j, j + wide)]
        )

    def couple(k):
        pair_ref[k, BLOCK:, :BLOCK] = dot_tn(a(k, k + 1), inv_ref[k])

    def pair(k):
        pair_ref[k, :BLOCK, :BLOCK] = inv_ref[k]
        pair_ref[k, BLOCK:, BLOCK:] = inv_ref[k + 1]
        pair_ref[k, :BLOCK, BLOCK:] = jnp.zeros((BLOCK, BLOCK), jnp.float32)
        pair_ref[k, BLOCK:, :BLOCK] = -dot(inv_ref[k + 1], pair_ref[k, BLOCK:, :BLOCK])

    def finish(k, wide, tile):
        factor = pair_ref[k] if wide == 2 else inv_ref[k]
        q_ref[tile, span(k, k + wide)] = dot_nt(x_ref[tile, span(k, k + wide)], factor)

    def project(first, last, tile):
        x_ref[tile, last * BLOCK:] = x_ref[tile, last * BLOCK:] - dot(
            q_ref[tile, span(first, last)], a_ref[span(first, last), last * BLOCK:]
        )

    def send(first, last):
        for b in range(first, last):
            stores[b].start()

    def after(k):
        if k + 1 == NBLK:
            return
        solve(k, k + 1)
        downdate(k + 1, k + 1, k, k + 1)
        first = k // 2 * 2
        if k % 2 == 0:
            soon.append(lambda: couple(k))
            if k + 2 < NBLK:
                soon.append(lambda: solve(k, k + 2))
                soon.append(lambda: downdate(k + 1, k + 2, k, k + 1))
                soon.append(lambda: downdate(k + 2, k + 2, k, k + 1))
            if k + 3 < NBLK:
                soon.append(lambda: solve(k, k + 3, NBLK - k - 3))
                soon.append(lambda: downdate(k + 1, k + 3, k, k + 1, NBLK - k - 3))
        else:
            if k + 2 < NBLK:
                soon.append(lambda: solve(k, k + 2, NBLK - k - 2))
                soon.append(lambda: downdate(k + 1, k + 2, first, k + 1, NBLK - k - 2))
                for i in range(k + 2, NBLK):
                    soon.append(lambda i=i: downdate(i, i, first, k + 1, NBLK - i))
            whenever.append(lambda: pair(first))
            for tile in tiles:
                whenever.append(lambda tile=tile: finish(first, 2, tile))
            whenever.append(lambda: send(first, k + 1))
            for tile in tiles:
                whenever.append(lambda tile=tile: project(first, k + 1, tile))

    def run(queue, count):
        for _ in range(min(count, len(queue))):
            queue.pop(0)()

    panels = BLOCK // PANEL
    for k in range(NBLK):
        work_ref[...] = a(k, k)
        state = {"left": panels}

        def between():
            run(soon, -(-len(soon) // max(state["left"] - 1, 1)))
            more = panels if k % 2 == 0 and k + 1 < NBLK else 0
            turns = state["left"] + more
            run(whenever, -(-len(whenever) // turns))
            state["left"] -= 1

        eliminate(work_ref, col_ref, between)
        run(soon, len(soon))
        inv_ref[k] = jnp.where(lower, work_ref[...], 0.0)
        if k == 1:
            for load in loads:
                load.wait()
        after(k)
    run(whenever, len(whenever))
    last = NBLK - 1
    for tile in tiles:
        finish(last, 1, tile)
    send(last, NBLK)
    for store in stores:
        store.wait()


def vmem():
    return pl.BlockSpec(memory_space=pltpu.VMEM)


def smem():
    return pl.BlockSpec(memory_space=pltpu.SMEM)


def anywhere():
    return pl.BlockSpec(memory_space=pl.ANY)


def finish_scratch(rows):
    bands = NBLK * BLOCK
    return [
        pltpu.VMEM((bands, bands), jnp.float32),
        pltpu.VMEM((NBLK, BLOCK, BLOCK), jnp.float32),
        pltpu.VMEM((NBLK, 2 * BLOCK, 2 * BLOCK), jnp.float32),
        pltpu.VMEM((rows, bands), jnp.float32),
        pltpu.VMEM((rows, bands), jnp.float32),
        pltpu.VMEM((BLOCK, BLOCK), jnp.float32),
        pltpu.VMEM((PANEL, PANEL, BLOCK), jnp.float32),
        pltpu.SemaphoreType.DMA((NBLK,)),
        pltpu.SemaphoreType.DMA((NBLK,)),
    ]


def local(psi, order):
    rows, bands = psi.shape
    size = lax.axis_size("grid")
    chips = size // 2
    scale = 1.0 / (rows * size)
    core = lax.axis_index("grid") % 2
    pairs = [(d, d ^ 1) for d in range(size)]
    groups = [list(range(c, size, 2)) for c in range(2)]
    half = SLOTS // 2
    chunk = half * BLOCK // chips

    gram = pl.pallas_call(
        lambda *refs: gram_kernel(scale, *refs),
        out_shape=pltpu.VMEM((SLOTS, BLOCK, BLOCK), jnp.float32),
        in_specs=[smem(), vmem()],
        out_specs=vmem(),
        scratch_shapes=[pltpu.VMEM((rows, bands), jnp.float32)],
        name="gram",
    )(order, psi)

    gram = gram.reshape(2, half, BLOCK, BLOCK)
    keep = lax.dynamic_index_in_dim(gram, core, 0, keepdims=False)
    send = lax.dynamic_index_in_dim(gram, 1 - core, 0, keepdims=False)
    both = keep + lax.ppermute(send, "grid", pairs)
    parts = lax.all_to_all(
        both.reshape(chips, chunk, BLOCK), "grid", 0, 0, axis_index_groups=groups, tiled=True
    )
    total = jnp.sum(parts, axis=0)
    mine = lax.all_to_all(
        jnp.broadcast_to(total[None], parts.shape), "grid", 0, 0, axis_index_groups=groups, tiled=True
    ).reshape(half, BLOCK, BLOCK)
    other = lax.ppermute(mine, "grid", pairs)
    mine = pltpu.with_memory_space_constraint(mine, pltpu.VMEM)
    other = pltpu.with_memory_space_constraint(other, pltpu.VMEM)

    return pl.pallas_call(
        finish_kernel,
        out_shape=jax.ShapeDtypeStruct((rows, bands), jnp.float32),
        in_specs=[smem(), smem(), vmem(), vmem(), anywhere()],
        out_specs=anywhere(),
        scratch_shapes=finish_scratch(rows),
        name="finish",
    )(core.astype(jnp.int32).reshape(1), order, mine, other, psi)


def solution(mesh):
    in_specs = (P(("frag", "grid"), None), P("frag"))
    out_specs = P(("frag", "grid"), None)
    return jax.shard_map(local, mesh=mesh, in_specs=in_specs, out_specs=out_specs, check_vma=False)
```

```python
import jax
import jax.numpy as jnp
from jax import lax
from jax.experimental import pallas as pl
from jax.experimental.pallas import tpu as pltpu
from jax.sharding import PartitionSpec as P

BLOCK = 128
NBLK = 5
PANEL = 32
SUB = 8
PANELS = BLOCK // PANEL
PAIRS = [(i, j) for i in range(NBLK) for j in range(i, NBLK)]
SLOT = {pair: slot for slot, pair in enumerate(PAIRS)}
SLOTS = 16
HIGHEST = lax.Precision.HIGHEST


def dot(left, right):
    return lax.dot_general(
        left, right, (((1,), (0,)), ((), ())), precision=HIGHEST, preferred_element_type=jnp.float32
    )


def dot_tn(left, right):
    return lax.dot_general(
        left, right, (((0,), (0,)), ((), ())), precision=HIGHEST, preferred_element_type=jnp.float32
    )


def dot_nt(left, right):
    return lax.dot_general(
        left, right, (((1,), (1,)), ((), ())), precision=HIGHEST, preferred_element_type=jnp.float32
    )


def span(first, last):
    return slice(first * BLOCK, last * BLOCK)


def block_copies(order_ref, far_ref, near_ref, sems, outward=False):
    copies = []
    for b in range(NBLK):
        start = pl.multiple_of(order_ref[b] * BLOCK, BLOCK)
        far = far_ref.at[:, pl.ds(start, BLOCK)]
        near = near_ref.at[:, span(b, b + 1)]
        copies.append(
            pltpu.make_async_copy(near, far, sems.at[b])
            if outward
            else pltpu.make_async_copy(far, near, sems.at[b])
        )
    return copies


def gram_kernel(scale, order_ref, psi_ref, out_ref, x_ref):
    for i in range(NBLK):
        start = pl.multiple_of(order_ref[i] * BLOCK, BLOCK)
        x_ref[:, span(i, i + 1)] = psi_ref[:, pl.ds(start, BLOCK)]
    for i in range(NBLK):
        row = dot_tn(x_ref[:, span(i, i + 1)], x_ref[:, i * BLOCK:]) * scale
        for j in range(i, NBLK):
            out_ref[SLOT[i, j]] = row[:, span(j - i, j - i + 1)]
    for extra in range(len(PAIRS), SLOTS):
        out_ref[extra] = jnp.zeros((BLOCK, BLOCK), jnp.float32)


def eliminate(work_ref, col_ref, after_panel):
    lane = lax.broadcasted_iota(jnp.int32, (SUB, BLOCK), 1)
    row = lax.broadcasted_iota(jnp.int32, (SUB, BLOCK), 0)
    pieces = PANEL // SUB
    for p in range(PANELS):
        r0 = p * PANEL
        low = r0 + PANEL
        for m in range(PANEL):
            top = m // SUB * SUB
            col_ref[m, top:, :] = jnp.broadcast_to(
                work_ref[r0 + top:low, r0 + m:r0 + m + 1], (PANEL - top, BLOCK)
            )
        inside = (lane >= r0) & (lane < low)
        part = []
        for q in range(pieces):
            unit = (lane == row + (r0 + q * SUB)).astype(jnp.float32)
            part.append(jnp.where(inside, unit, work_ref[r0 + q * SUB:r0 + (q + 1) * SUB, :]))
        column = {
            (m, q): col_ref[m, q * SUB:(q + 1) * SUB, :]
            for m in range(PANEL)
            for q in range(m // SUB, pieces)
        }
        diag = [jnp.ones((SUB, BLOCK), jnp.float32)] * pieces
        for k in range(PANEL):
            kq, ks = divmod(k, SUB)
            pivot = column[k, kq][ks:ks + 1, :]
            inverse = 1.0 / pivot
            diag[kq] = jnp.where(row == ks, pivot, diag[kq])
            factor = {q: column[k, q] * inverse for q in range(kq, pieces)}
            for m in range(k + 1, PANEL):
                mq, ms = divmod(m, SUB)
                entry = column[k, mq][ms:ms + 1, :]
                for q in range(mq, pieces):
                    column[m, q] = column[m, q] - factor[q] * entry
            lead = part[kq][ks:ks + 1, :]
            part[kq] = part[kq] - jnp.where(row > ks, factor[kq], 0.0) * lead
            for q in range(kq + 1, pieces):
                part[q] = part[q] - factor[q] * lead
        work_ref[r0:low, :] = jnp.concatenate(
            [part[q] * lax.rsqrt(diag[q]) for q in range(pieces)], axis=0
        )
        if low < BLOCK:
            turned = jnp.concatenate(part, axis=0).T
            scaled = jnp.concatenate([part[q] * (1.0 / diag[q]) for q in range(pieces)], axis=0)
            for first, last in ((low, low + PANEL), (low + PANEL, BLOCK)):
                if first < last:
                    rest = lax.broadcasted_iota(jnp.int32, (last - first, BLOCK), 1)
                    kept = jnp.where((rest >= r0) & (rest < low), 0.0, work_ref[first:last, :])
                    work_ref[first:last, :] = kept - dot(turned[first:last, :], scaled)
        after_panel(p)


def finish_kernel(
    core_ref, order_ref, mine_ref, other_ref, psi_ref, out_ref,
    a_ref, inv_ref, pair_ref, x_ref, q_ref, work_ref, next_ref, col_ref, in_sems, out_sems,
):
    loads = block_copies(order_ref, psi_ref, x_ref, in_sems)
    stores = block_copies(order_ref, out_ref, q_ref, out_sems, outward=True)
    final = NBLK - 1
    for load in loads:
        load.start()
    core = core_ref[0]
    half = SLOTS // 2
    for slot, (i, j) in enumerate(PAIRS):
        own = core == slot // half
        a_ref[span(i, i + 1), span(j, j + 1)] = jnp.where(
            own, mine_ref[slot % half], other_ref[slot % half]
        )
    lower = (
        lax.broadcasted_iota(jnp.int32, (BLOCK, BLOCK), 0)
        >= lax.broadcasted_iota(jnp.int32, (BLOCK, BLOCK), 1)
    )
    rows = x_ref.shape[0]
    tiles = [slice(r, r + BLOCK) for r in range(0, rows, BLOCK)]
    soon, whenever = [], []
    where_to = pl.multiple_of(order_ref[final] * BLOCK, BLOCK)
    stores = stores[:final] + [
        pltpu.make_async_copy(
            q_ref.at[tile, span(final, NBLK)],
            out_ref.at[tile, pl.ds(where_to, BLOCK)],
            out_sems.at[final + t],
        )
        for t, tile in enumerate(tiles)
    ]

    def a(i, j, wide=1):
        return a_ref[span(i, i + 1), span(j, j + wide)]

    def solve(k, j, wide=1):
        a_ref[span(k, k + 1), span(j, j + wide)] = dot(inv_ref[k], a(k, j, wide))

    def downdate(i, j, first, last, wide=1):
        ks = span(first, last)
        a_ref[span(i, i + 1), span(j, j + wide)] = a(i, j, wide) - dot_tn(
            a_ref[ks, span(i, i + 1)], a_ref[ks, span(j, j + wide)]
        )

    def couple(k):
        pair_ref[k, BLOCK:, :BLOCK] = dot_tn(a(k, k + 1), inv_ref[k])

    def pair(k):
        pair_ref[k, :BLOCK, :BLOCK] = inv_ref[k]
        pair_ref[k, BLOCK:, BLOCK:] = inv_ref[k + 1]
        pair_ref[k, :BLOCK, BLOCK:] = jnp.zeros((BLOCK, BLOCK), jnp.float32)
        pair_ref[k, BLOCK:, :BLOCK] = -dot(inv_ref[k + 1], pair_ref[k, BLOCK:, :BLOCK])

    def finish(k, wide, tile):
        factor = pair_ref[k] if wide == 2 else inv_ref[k]
        q_ref[tile, span(k, k + wide)] = dot_nt(x_ref[tile, span(k, k + wide)], factor)

    def project(first, last, tile):
        x_ref[tile, last * BLOCK:] = x_ref[tile, last * BLOCK:] - dot(
            q_ref[tile, span(first, last)], a_ref[span(first, last), last * BLOCK:]
        )

    def send(first, last):
        for b in range(first, last):
            stores[b].start()

    def solve_rows(k, p, work):
        rows = slice(k * BLOCK + p * PANEL, k * BLOCK + (p + 1) * PANEL)
        lane = lax.broadcasted_iota(jnp.int32, (PANEL, BLOCK), 1)
        left = jnp.where(lane < (p + 1) * PANEL, work[p * PANEL:(p + 1) * PANEL, :], 0.0)
        value = dot(left, original[...])
        a_ref[rows, span(k + 1, k + 2)] = value
        return value

    def after(k):
        first = k // 2 * 2
        if k + 1 == NBLK:
            return
        if k % 2 == 0:
            soon.append(lambda: couple(k))
            if k + 2 < NBLK:
                soon.append(lambda: solve(k, k + 2))
                soon.append(lambda: downdate(k + 1, k + 2, k, k + 1))
                soon.append(lambda: downdate(k + 2, k + 2, k, k + 1))
            if k + 3 < NBLK:
                soon.append(lambda: solve(k, k + 3, NBLK - k - 3))
                soon.append(lambda: downdate(k + 1, k + 3, k, k + 1, NBLK - k - 3))
        else:
            if k + 2 < NBLK:
                soon.append(lambda: solve(k, k + 2, NBLK - k - 2))
                soon.append(lambda: downdate(k + 1, k + 2, first, k + 1, NBLK - k - 2))
                for i in range(k + 2, NBLK):
                    soon.append(lambda i=i: downdate(i, i, first, k + 1, NBLK - i))
            whenever.append(lambda: pair(first))
            for tile in tiles:
                whenever.append(lambda tile=tile: finish(first, 2, tile))
            whenever.append(lambda: send(first, k + 1))
            for tile in tiles:
                whenever.append(lambda tile=tile: project(first, k + 1, tile))

    def run(queue, count):
        for _ in range(min(count, len(queue))):
            queue.pop(0)()

    work_ref[0] = a(0, 0)
    for k in range(NBLK):
        work = work_ref.at[k % 2]
        following = work_ref.at[1 - k % 2]
        original = next_ref.at[k % 2]
        more = k + 1 < NBLK
        early = (PANELS - 1) * PANEL

        def after_panel(p):
            if p == PANELS - 1:
                return
            left = PANELS - 1 - p
            run(soon, -(-len(soon) // max(left - 1, 1)))
            if p == PANELS - 2:
                run(soon, len(soon))
                if more:
                    original[...] = a(k, k + 1)
                    for done in range(PANELS - 1):
                        solve_rows(k, done, work)
                    solved = a_ref[k * BLOCK:k * BLOCK + early, span(k + 1, k + 2)]
                    following[...] = a(k + 1, k + 1) - dot_tn(solved, solved)
            turns = left + (PANELS - 1 if k % 2 == 0 and more else 0)
            run(whenever, -(-len(whenever) // turns))

        eliminate(work, col_ref, after_panel)
        if more:
            value = solve_rows(k, PANELS - 1, work)
            turned = value.T
            for first, last in ((0, PANEL), (PANEL, BLOCK)):
                following[first:last, :] = following[first:last, :] - dot(turned[first:last, :], value)
        inv_ref[k] = jnp.where(lower, work[...], 0.0)
        if k == 1:
            for load in loads:
                load.wait()
        after(k)
    run(whenever, len(whenever))
    for t, tile in enumerate(tiles):
        finish(final, 1, tile)
        stores[final + t].start()
    for store in stores:
        store.wait()


def vmem():
    return pl.BlockSpec(memory_space=pltpu.VMEM)


def smem():
    return pl.BlockSpec(memory_space=pltpu.SMEM)


def anywhere():
    return pl.BlockSpec(memory_space=pl.ANY)


def finish_scratch(rows):
    bands = NBLK * BLOCK
    return [
        pltpu.VMEM((bands, bands), jnp.float32),
        pltpu.VMEM((NBLK, BLOCK, BLOCK), jnp.float32),
        pltpu.VMEM((NBLK, 2 * BLOCK, 2 * BLOCK), jnp.float32),
        pltpu.VMEM((rows, bands), jnp.float32),
        pltpu.VMEM((rows, bands), jnp.float32),
        pltpu.VMEM((2, BLOCK, BLOCK), jnp.float32),
        pltpu.VMEM((2, BLOCK, BLOCK), jnp.float32),
        pltpu.VMEM((PANEL, PANEL, BLOCK), jnp.float32),
        pltpu.SemaphoreType.DMA((NBLK,)),
        pltpu.SemaphoreType.DMA((NBLK - 1 + rows // BLOCK,)),
    ]


def local(psi, order):
    rows, bands = psi.shape
    size = lax.axis_size("grid")
    chips = size // 2
    scale = 1.0 / (rows * size)
    core = lax.axis_index("grid") % 2
    pairs = [(d, d ^ 1) for d in range(size)]
    groups = [list(range(c, size, 2)) for c in range(2)]
    half = SLOTS // 2
    chunk = half * BLOCK // chips

    gram = pl.pallas_call(
        lambda *refs: gram_kernel(scale, *refs),
        out_shape=pltpu.VMEM((SLOTS, BLOCK, BLOCK), jnp.float32),
        in_specs=[smem(), vmem()],
        out_specs=vmem(),
        scratch_shapes=[pltpu.VMEM((rows, bands), jnp.float32)],
        name="gram",
    )(order, psi)

    gram = gram.reshape(2, half, BLOCK, BLOCK)
    keep = lax.dynamic_index_in_dim(gram, core, 0, keepdims=False)
    send = lax.dynamic_index_in_dim(gram, 1 - core, 0, keepdims=False)
    both = keep + lax.ppermute(send, "grid", pairs)
    parts = lax.all_to_all(
        both.reshape(chips, chunk, BLOCK), "grid", 0, 0, axis_index_groups=groups, tiled=True
    )
    total = jnp.sum(parts, axis=0)
    mine = lax.all_to_all(
        jnp.broadcast_to(total[None], parts.shape), "grid", 0, 0, axis_index_groups=groups, tiled=True
    ).reshape(half, BLOCK, BLOCK)
    other = lax.ppermute(mine, "grid", pairs)
    mine = pltpu.with_memory_space_constraint(mine, pltpu.VMEM)
    other = pltpu.with_memory_space_constraint(other, pltpu.VMEM)

    return pl.pallas_call(
        finish_kernel,
        out_shape=jax.ShapeDtypeStruct((rows, bands), jnp.float32),
        in_specs=[smem(), smem(), vmem(), vmem(), anywhere()],
        out_specs=anywhere(),
        scratch_shapes=finish_scratch(rows),
        name="finish",
    )(core.astype(jnp.int32).reshape(1), order, mine, other, psi)


def solution(mesh):
    in_specs = (P(("frag", "grid"), None), P("frag"))
    out_specs = P(("frag", "grid"), None)
    return jax.shard_map(local, mesh=mesh, in_specs=in_specs, out_specs=out_specs, check_vma=False)
```

```python
import jax
import jax.numpy as jnp
from jax import lax
from jax.experimental import pallas as pl
from jax.experimental.pallas import tpu as pltpu
from jax.sharding import PartitionSpec as P

BLOCK = 128
NBLK = 5
PANEL = 32
SUB = 8
PANELS = BLOCK // PANEL
PAIRS = [(i, j) for i in range(NBLK) for j in range(i, NBLK)]
SLOT = {pair: slot for slot, pair in enumerate(PAIRS)}
SLOTS = 16
HIGHEST = lax.Precision.HIGHEST


def dot(left, right):
    return lax.dot_general(
        left, right, (((1,), (0,)), ((), ())), precision=HIGHEST, preferred_element_type=jnp.float32
    )


def dot_tn(left, right):
    return lax.dot_general(
        left, right, (((0,), (0,)), ((), ())), precision=HIGHEST, preferred_element_type=jnp.float32
    )


def dot_nt(left, right):
    return lax.dot_general(
        left, right, (((1,), (1,)), ((), ())), precision=HIGHEST, preferred_element_type=jnp.float32
    )


def span(first, last):
    return slice(first * BLOCK, last * BLOCK)


def block_copies(order_ref, far_ref, near_ref, sems, count, outward=False):
    copies = []
    for b in range(count):
        start = pl.multiple_of(order_ref[b] * BLOCK, BLOCK)
        far = far_ref.at[:, pl.ds(start, BLOCK)]
        near = near_ref.at[:, span(b, b + 1)]
        copies.append(
            pltpu.make_async_copy(near, far, sems.at[b])
            if outward
            else pltpu.make_async_copy(far, near, sems.at[b])
        )
    return copies


def gram_kernel(scale, order_ref, psi_ref, out_ref, x_ref):
    for i in range(NBLK):
        start = pl.multiple_of(order_ref[i] * BLOCK, BLOCK)
        x_ref[:, span(i, i + 1)] = psi_ref[:, pl.ds(start, BLOCK)]
    for i in range(NBLK):
        row = dot_tn(x_ref[:, span(i, i + 1)], x_ref[:, i * BLOCK:]) * scale
        for j in range(i, NBLK):
            out_ref[SLOT[i, j]] = row[:, span(j - i, j - i + 1)]
    out_ref[SLOTS - 1] = out_ref[0]


def eliminate(work_ref, col_ref, row_ref, after_panel):
    lane = lax.broadcasted_iota(jnp.int32, (SUB, BLOCK), 1)
    row = lax.broadcasted_iota(jnp.int32, (SUB, BLOCK), 0)
    pieces = PANEL // SUB
    for p in range(PANELS):
        r0 = p * PANEL
        low = r0 + PANEL
        for m in range(PANEL):
            top = m // SUB * SUB
            col_ref[m, top:, :] = jnp.broadcast_to(
                work_ref[r0 + top:low, r0 + m:r0 + m + 1], (PANEL - top, BLOCK)
            )
        inside = (lane >= r0) & (lane < low)
        part = []
        for q in range(pieces):
            unit = (lane == row + (r0 + q * SUB)).astype(jnp.float32)
            part.append(jnp.where(inside, unit, work_ref[r0 + q * SUB:r0 + (q + 1) * SUB, :]))
        diag = [jnp.ones((SUB, BLOCK), jnp.float32)] * pieces
        factors = {}
        for group in range(pieces):
            column = {}
            for m in range(group * SUB, (group + 1) * SUB):
                for q in range(group, pieces):
                    value = col_ref[m, q * SUB:(q + 1) * SUB, :]
                    for k in range(group * SUB):
                        value = value - factors[k, q] * row_ref[k, m:m + 1, :]
                    column[m, q] = value
            for k in range(group * SUB, (group + 1) * SUB):
                ks = k % SUB
                pivot = column[k, group][ks:ks + 1, :]
                inverse = 1.0 / pivot
                diag[group] = jnp.where(row == ks, pivot, diag[group])
                for q in range(group, pieces):
                    factors[k, q] = column[k, q] * inverse
                for q in range(group + 1, pieces):
                    row_ref[k, q * SUB:(q + 1) * SUB, :] = column[k, q]
                for m in range(k + 1, (group + 1) * SUB):
                    entry = column[k, group][m % SUB:m % SUB + 1, :]
                    for q in range(group, pieces):
                        column[m, q] = column[m, q] - factors[k, q] * entry
                lead = part[group][ks:ks + 1, :]
                part[group] = part[group] - jnp.where(row > ks, factors[k, group], 0.0) * lead
                for q in range(group + 1, pieces):
                    part[q] = part[q] - factors[k, q] * lead
        work_ref[r0:low, :] = jnp.concatenate(
            [part[q] * lax.rsqrt(diag[q]) for q in range(pieces)], axis=0
        )
        if low < BLOCK:
            turned = jnp.concatenate(part, axis=0).T
            scaled = jnp.concatenate([part[q] * (1.0 / diag[q]) for q in range(pieces)], axis=0)
            for first, last in ((low, low + PANEL), (low + PANEL, BLOCK)):
                if first < last:
                    rest = lax.broadcasted_iota(jnp.int32, (last - first, BLOCK), 1)
                    kept = jnp.where((rest >= r0) & (rest < low), 0.0, work_ref[first:last, :])
                    work_ref[first:last, :] = kept - dot(turned[first:last, :], scaled)
        after_panel(p)


def lead_kernel(core_ref, mine_ref, out_ref, work_ref, col_ref, row_ref):
    work_ref[...] = jnp.where(core_ref[0] == 0, mine_ref[0], mine_ref[SLOTS // 2 - 1])
    eliminate(work_ref, col_ref, row_ref, lambda p: None)
    out_ref[...] = work_ref[...]


def finish_kernel(
    core_ref, order_ref, lead_ref, mine_ref, other_ref, psi_ref, out_ref,
    a_ref, inv_ref, pair_ref, x_ref, q_ref, work_ref, next_ref, col_ref, row_ref, in_sems, out_sems,
):
    loads = block_copies(order_ref, psi_ref, x_ref, in_sems, NBLK)
    final = NBLK - 1
    stores = block_copies(order_ref, out_ref, q_ref, out_sems, final, outward=True)
    for load in loads:
        load.start()
    core = core_ref[0]
    half = SLOTS // 2
    for slot, (i, j) in enumerate(PAIRS):
        own = core == slot // half
        a_ref[span(i, i + 1), span(j, j + 1)] = jnp.where(
            own, mine_ref[slot % half], other_ref[slot % half]
        )
    lower = (
        lax.broadcasted_iota(jnp.int32, (BLOCK, BLOCK), 0)
        >= lax.broadcasted_iota(jnp.int32, (BLOCK, BLOCK), 1)
    )
    rows = x_ref.shape[0]
    tiles = [slice(r, r + BLOCK) for r in range(0, rows, BLOCK)]
    soon, whenever = [], []
    where_to = pl.multiple_of(order_ref[final] * BLOCK, BLOCK)
    stores = stores + [
        pltpu.make_async_copy(
            q_ref.at[tile, span(final, NBLK)],
            out_ref.at[tile, pl.ds(where_to, BLOCK)],
            out_sems.at[final + t],
        )
        for t, tile in enumerate(tiles)
    ]

    def a(i, j, wide=1):
        return a_ref[span(i, i + 1), span(j, j + wide)]

    def solve(k, j, wide=1):
        a_ref[span(k, k + 1), span(j, j + wide)] = dot(inv_ref[k], a(k, j, wide))

    def downdate(i, j, first, last, wide=1):
        ks = span(first, last)
        a_ref[span(i, i + 1), span(j, j + wide)] = a(i, j, wide) - dot_tn(
            a_ref[ks, span(i, i + 1)], a_ref[ks, span(j, j + wide)]
        )

    def couple(k):
        pair_ref[k, BLOCK:, :BLOCK] = dot_tn(a(k, k + 1), inv_ref[k])

    def pair(k):
        pair_ref[k, :BLOCK, :BLOCK] = inv_ref[k]
        pair_ref[k, BLOCK:, BLOCK:] = inv_ref[k + 1]
        pair_ref[k, :BLOCK, BLOCK:] = jnp.zeros((BLOCK, BLOCK), jnp.float32)
        pair_ref[k, BLOCK:, :BLOCK] = -dot(inv_ref[k + 1], pair_ref[k, BLOCK:, :BLOCK])

    def finish(k, wide, tile):
        factor = pair_ref[k] if wide == 2 else inv_ref[k]
        q_ref[tile, span(k, k + wide)] = dot_nt(x_ref[tile, span(k, k + wide)], factor)

    def project(first, last, tile):
        x_ref[tile, last * BLOCK:] = x_ref[tile, last * BLOCK:] - dot(
            q_ref[tile, span(first, last)], a_ref[span(first, last), last * BLOCK:]
        )

    def send(first, last):
        for b in range(first, last):
            stores[b].start()

    def solve_rows(k, p, work):
        rows = slice(k * BLOCK + p * PANEL, k * BLOCK + (p + 1) * PANEL)
        lane = lax.broadcasted_iota(jnp.int32, (PANEL, BLOCK), 1)
        left = jnp.where(lane < (p + 1) * PANEL, work[p * PANEL:(p + 1) * PANEL, :], 0.0)
        value = dot(left, original[...])
        a_ref[rows, span(k + 1, k + 2)] = value
        return value

    def after(k):
        first = k // 2 * 2
        if k + 1 == NBLK:
            return
        if k % 2 == 0:
            soon.append(lambda: couple(k))
            if k + 2 < NBLK:
                soon.append(lambda: solve(k, k + 2))
                soon.append(lambda: downdate(k + 1, k + 2, k, k + 1))
                soon.append(lambda: downdate(k + 2, k + 2, k, k + 1))
            if k + 3 < NBLK:
                soon.append(lambda: solve(k, k + 3, NBLK - k - 3))
                soon.append(lambda: downdate(k + 1, k + 3, k, k + 1, NBLK - k - 3))
        else:
            if k + 2 < NBLK:
                soon.append(lambda: solve(k, k + 2, NBLK - k - 2))
                soon.append(lambda: downdate(k + 1, k + 2, first, k + 1, NBLK - k - 2))
                for i in range(k + 2, NBLK):
                    soon.append(lambda i=i: downdate(i, i, first, k + 1, NBLK - i))
            whenever.append(lambda: pair(first))
            for tile in tiles:
                whenever.append(lambda tile=tile: finish(first, 2, tile))
            whenever.append(lambda: send(first, k + 1))
            for tile in tiles:
                whenever.append(lambda tile=tile: project(first, k + 1, tile))

    def run(queue, count):
        for _ in range(min(count, len(queue))):
            queue.pop(0)()

    inv_ref[0] = jnp.where(lower, lead_ref[...], 0.0)
    solve(0, 1)
    turned = a(0, 1).T
    for first, last in ((0, PANEL), (PANEL, BLOCK)):
        work_ref[1, first:last, :] = a_ref[BLOCK + first:BLOCK + last, span(1, 2)] - dot(
            turned[first:last, :], a(0, 1)
        )
    after(0)
    for k in range(1, NBLK):
        work = work_ref.at[k % 2]
        following = work_ref.at[1 - k % 2]
        original = next_ref.at[k % 2]
        more = k + 1 < NBLK
        early = (PANELS - 1) * PANEL

        def after_panel(p):
            if p == PANELS - 1:
                return
            left = PANELS - 1 - p
            run(soon, -(-len(soon) // max(left - 1, 1)))
            if p == PANELS - 2:
                run(soon, len(soon))
                if more:
                    original[...] = a(k, k + 1)
                    for done in range(PANELS - 1):
                        solve_rows(k, done, work)
                    solved = a_ref[k * BLOCK:k * BLOCK + early, span(k + 1, k + 2)]
                    following[...] = a(k + 1, k + 1) - dot_tn(solved, solved)
            turns = left + (PANELS - 1 if k % 2 == 0 and more else 0)
            run(whenever, -(-len(whenever) // turns))

        eliminate(work, col_ref, row_ref, after_panel)
        if more:
            value = solve_rows(k, PANELS - 1, work)
            turned = value.T
            for first, last in ((0, PANEL), (PANEL, BLOCK)):
                following[first:last, :] = following[first:last, :] - dot(turned[first:last, :], value)
        inv_ref[k] = jnp.where(lower, work[...], 0.0)
        if k == 1:
            for load in loads:
                load.wait()
        after(k)
    run(whenever, len(whenever))
    for t, tile in enumerate(tiles):
        finish(final, 1, tile)
        stores[final + t].start()
    for store in stores:
        store.wait()


def vmem():
    return pl.BlockSpec(memory_space=pltpu.VMEM)


def smem():
    return pl.BlockSpec(memory_space=pltpu.SMEM)


def anywhere():
    return pl.BlockSpec(memory_space=pl.ANY)


def finish_scratch(rows):
    bands = NBLK * BLOCK
    return [
        pltpu.VMEM((bands, bands), jnp.float32),
        pltpu.VMEM((NBLK, BLOCK, BLOCK), jnp.float32),
        pltpu.VMEM((NBLK, 2 * BLOCK, 2 * BLOCK), jnp.float32),
        pltpu.VMEM((rows, bands), jnp.float32),
        pltpu.VMEM((rows, bands), jnp.float32),
        pltpu.VMEM((2, BLOCK, BLOCK), jnp.float32),
        pltpu.VMEM((2, BLOCK, BLOCK), jnp.float32),
        pltpu.VMEM((PANEL, PANEL, BLOCK), jnp.float32),
        pltpu.VMEM((PANEL, PANEL, BLOCK), jnp.float32),
        pltpu.SemaphoreType.DMA((NBLK,)),
        pltpu.SemaphoreType.DMA((NBLK - 1 + rows // BLOCK,)),
    ]


def local(psi, order):
    rows, bands = psi.shape
    size = lax.axis_size("grid")
    chips = size // 2
    scale = 1.0 / (rows * size)
    core = lax.axis_index("grid") % 2
    pairs = [(d, d ^ 1) for d in range(size)]
    groups = [list(range(c, size, 2)) for c in range(2)]
    half = SLOTS // 2
    chunk = half * BLOCK // chips

    gram = pl.pallas_call(
        lambda *refs: gram_kernel(scale, *refs),
        out_shape=pltpu.VMEM((SLOTS, BLOCK, BLOCK), jnp.float32),
        in_specs=[smem(), vmem()],
        out_specs=vmem(),
        scratch_shapes=[pltpu.VMEM((rows, bands), jnp.float32)],
        name="gram",
    )(order, psi)

    gram = gram.reshape(2, half, BLOCK, BLOCK)
    keep = lax.dynamic_index_in_dim(gram, core, 0, keepdims=False)
    send = lax.dynamic_index_in_dim(gram, 1 - core, 0, keepdims=False)
    both = keep + lax.ppermute(send, "grid", pairs)
    parts = lax.all_to_all(
        both.reshape(chips, chunk, BLOCK), "grid", 0, 0, axis_index_groups=groups, tiled=True
    )
    total = jnp.sum(parts, axis=0)
    mine = lax.all_to_all(
        jnp.broadcast_to(total[None], parts.shape), "grid", 0, 0, axis_index_groups=groups, tiled=True
    ).reshape(half, BLOCK, BLOCK)
    other = lax.ppermute(mine, "grid", pairs)
    mine = pltpu.with_memory_space_constraint(mine, pltpu.VMEM)
    other = pltpu.with_memory_space_constraint(other, pltpu.VMEM)

    core = core.astype(jnp.int32).reshape(1)
    lead = pl.pallas_call(
        lead_kernel,
        out_shape=pltpu.VMEM((BLOCK, BLOCK), jnp.float32),
        in_specs=[smem(), vmem()],
        out_specs=vmem(),
        scratch_shapes=[
            pltpu.VMEM((BLOCK, BLOCK), jnp.float32),
            pltpu.VMEM((PANEL, PANEL, BLOCK), jnp.float32),
            pltpu.VMEM((PANEL, PANEL, BLOCK), jnp.float32),
        ],
        name="lead",
    )(core, mine)
    lead = pltpu.with_memory_space_constraint(lead, pltpu.VMEM)
    return pl.pallas_call(
        finish_kernel,
        out_shape=jax.ShapeDtypeStruct((rows, bands), jnp.float32),
        in_specs=[smem(), smem(), vmem(), vmem(), vmem(), anywhere()],
        out_specs=anywhere(),
        scratch_shapes=finish_scratch(rows),
        name="finish",
    )(core, order, lead, mine, other, psi)


def solution(mesh):
    in_specs = (P(("frag", "grid"), None), P("frag"))
    out_specs = P(("frag", "grid"), None)
    return jax.shard_map(local, mesh=mesh, in_specs=in_specs, out_specs=out_specs, check_vma=False)
```

```python
import jax
import jax.numpy as jnp
from jax import lax
from jax.experimental import pallas as pl
from jax.experimental.pallas import tpu as pltpu
from jax.sharding import PartitionSpec as P

BLOCK = 128
NBLK = 5
PANEL = 32
SUB = 8
PANELS = BLOCK // PANEL
PAIRS = [(i, j) for i in range(NBLK) for j in range(i, NBLK)]
SLOT = {pair: slot for slot, pair in enumerate(PAIRS)}
SLOTS = 16
HIGHEST = lax.Precision.HIGHEST


def dot(left, right):
    return lax.dot_general(
        left, right, (((1,), (0,)), ((), ())), precision=HIGHEST, preferred_element_type=jnp.float32
    )


def dot_tn(left, right):
    return lax.dot_general(
        left, right, (((0,), (0,)), ((), ())), precision=HIGHEST, preferred_element_type=jnp.float32
    )


def dot_nt(left, right):
    return lax.dot_general(
        left, right, (((1,), (1,)), ((), ())), precision=HIGHEST, preferred_element_type=jnp.float32
    )


def span(first, last):
    return slice(first * BLOCK, last * BLOCK)


def block_copies(order_ref, far_ref, near_ref, sems, count, outward=False):
    copies = []
    for b in range(count):
        start = pl.multiple_of(order_ref[b] * BLOCK, BLOCK)
        far = far_ref.at[:, pl.ds(start, BLOCK)]
        near = near_ref.at[:, span(b, b + 1)]
        copies.append(
            pltpu.make_async_copy(near, far, sems.at[b])
            if outward
            else pltpu.make_async_copy(far, near, sems.at[b])
        )
    return copies


def gram_half(scale, half, x_ref, out_ref):
    first = half * (SLOTS // 2)
    held = PAIRS[first:first + SLOTS // 2]
    for i in range(NBLK):
        js = [j for row, j in held if row == i]
        if js:
            row = dot_tn(x_ref[:, span(i, i + 1)], x_ref[:, span(js[0], js[-1] + 1)]) * scale
            for at, j in enumerate(js):
                out_ref[SLOT[i, j] - first] = row[:, span(at, at + 1)]
    if half == 1:
        lead = x_ref[:, span(0, 1)]
        out_ref[SLOTS // 2 - 1] = dot_tn(lead, lead) * scale


def send_kernel(scale, core_ref, order_ref, psi_ref, out_ref, x_ref):
    for i in range(NBLK):
        start = pl.multiple_of(order_ref[i] * BLOCK, BLOCK)
        x_ref[:, span(i, i + 1)] = psi_ref[:, pl.ds(start, BLOCK)]
    for core in range(2):
        pl.when(core_ref[0] == core)(lambda: gram_half(scale, 1 - core, x_ref, out_ref))


def keep_kernel(scale, core_ref, x_ref, out_ref):
    for core in range(2):
        pl.when(core_ref[0] == core)(lambda: gram_half(scale, core, x_ref, out_ref))


def eliminate(work_ref, col_ref, row_ref, after_panel):
    lane = lax.broadcasted_iota(jnp.int32, (SUB, BLOCK), 1)
    row = lax.broadcasted_iota(jnp.int32, (SUB, BLOCK), 0)
    pieces = PANEL // SUB
    for p in range(PANELS):
        r0 = p * PANEL
        low = r0 + PANEL
        for m in range(PANEL):
            top = m // SUB * SUB
            col_ref[m, top:, :] = jnp.broadcast_to(
                work_ref[r0 + top:low, r0 + m:r0 + m + 1], (PANEL - top, BLOCK)
            )
        inside = (lane >= r0) & (lane < low)
        part = []
        for q in range(pieces):
            unit = (lane == row + (r0 + q * SUB)).astype(jnp.float32)
            part.append(jnp.where(inside, unit, work_ref[r0 + q * SUB:r0 + (q + 1) * SUB, :]))
        diag = [jnp.ones((SUB, BLOCK), jnp.float32)] * pieces
        factors = {}
        for group in range(pieces):
            column = {}
            for m in range(group * SUB, (group + 1) * SUB):
                for q in range(group, pieces):
                    value = col_ref[m, q * SUB:(q + 1) * SUB, :]
                    for k in range(group * SUB):
                        value = value - factors[k, q] * row_ref[k, m:m + 1, :]
                    column[m, q] = value
            for k in range(group * SUB, (group + 1) * SUB):
                ks = k % SUB
                pivot = column[k, group][ks:ks + 1, :]
                inverse = 1.0 / pivot
                diag[group] = jnp.where(row == ks, pivot, diag[group])
                for q in range(group, pieces):
                    factors[k, q] = column[k, q] * inverse
                for q in range(group + 1, pieces):
                    row_ref[k, q * SUB:(q + 1) * SUB, :] = column[k, q]
                for m in range(k + 1, (group + 1) * SUB):
                    entry = column[k, group][m % SUB:m % SUB + 1, :]
                    for q in range(group, pieces):
                        column[m, q] = column[m, q] - factors[k, q] * entry
                lead = part[group][ks:ks + 1, :]
                part[group] = part[group] - jnp.where(row > ks, factors[k, group], 0.0) * lead
                for q in range(group + 1, pieces):
                    part[q] = part[q] - factors[k, q] * lead
        work_ref[r0:low, :] = jnp.concatenate(
            [part[q] * lax.rsqrt(diag[q]) for q in range(pieces)], axis=0
        )
        if low < BLOCK:
            turned = jnp.concatenate(part, axis=0).T
            scaled = jnp.concatenate([part[q] * (1.0 / diag[q]) for q in range(pieces)], axis=0)
            for first, last in ((low, low + PANEL), (low + PANEL, BLOCK)):
                if first < last:
                    rest = lax.broadcasted_iota(jnp.int32, (last - first, BLOCK), 1)
                    kept = jnp.where((rest >= r0) & (rest < low), 0.0, work_ref[first:last, :])
                    work_ref[first:last, :] = kept - dot(turned[first:last, :], scaled)
        after_panel(p)


def lead_kernel(core_ref, mine_ref, out_ref, work_ref, col_ref, row_ref):
    work_ref[...] = jnp.where(core_ref[0] == 0, mine_ref[0], mine_ref[SLOTS // 2 - 1])
    eliminate(work_ref, col_ref, row_ref, lambda p: None)
    out_ref[...] = work_ref[...]


def finish_kernel(
    core_ref, order_ref, lead_ref, mine_ref, other_ref, psi_ref, out_ref,
    a_ref, inv_ref, pair_ref, x_ref, q_ref, work_ref, next_ref, col_ref, row_ref, in_sems, out_sems,
):
    loads = block_copies(order_ref, psi_ref, x_ref, in_sems, NBLK)
    final = NBLK - 1
    stores = block_copies(order_ref, out_ref, q_ref, out_sems, final, outward=True)
    for load in loads:
        load.start()
    core = core_ref[0]
    half = SLOTS // 2
    for slot, (i, j) in enumerate(PAIRS):
        own = core == slot // half
        a_ref[span(i, i + 1), span(j, j + 1)] = jnp.where(
            own, mine_ref[slot % half], other_ref[slot % half]
        )
    lower = (
        lax.broadcasted_iota(jnp.int32, (BLOCK, BLOCK), 0)
        >= lax.broadcasted_iota(jnp.int32, (BLOCK, BLOCK), 1)
    )
    rows = x_ref.shape[0]
    tiles = [slice(r, r + BLOCK) for r in range(0, rows, BLOCK)]
    soon, whenever = [], []
    where_to = pl.multiple_of(order_ref[final] * BLOCK, BLOCK)
    stores = stores + [
        pltpu.make_async_copy(
            q_ref.at[tile, span(final, NBLK)],
            out_ref.at[tile, pl.ds(where_to, BLOCK)],
            out_sems.at[final + t],
        )
        for t, tile in enumerate(tiles)
    ]

    def a(i, j, wide=1):
        return a_ref[span(i, i + 1), span(j, j + wide)]

    def solve(k, j, wide=1):
        a_ref[span(k, k + 1), span(j, j + wide)] = dot(inv_ref[k], a(k, j, wide))

    def downdate(i, j, first, last, wide=1):
        ks = span(first, last)
        a_ref[span(i, i + 1), span(j, j + wide)] = a(i, j, wide) - dot_tn(
            a_ref[ks, span(i, i + 1)], a_ref[ks, span(j, j + wide)]
        )

    def couple(k):
        pair_ref[k, BLOCK:, :BLOCK] = dot_tn(a(k, k + 1), inv_ref[k])

    def pair(k):
        pair_ref[k, :BLOCK, :BLOCK] = inv_ref[k]
        pair_ref[k, BLOCK:, BLOCK:] = inv_ref[k + 1]
        pair_ref[k, :BLOCK, BLOCK:] = jnp.zeros((BLOCK, BLOCK), jnp.float32)
        pair_ref[k, BLOCK:, :BLOCK] = -dot(inv_ref[k + 1], pair_ref[k, BLOCK:, :BLOCK])

    def finish(k, wide, tile):
        factor = pair_ref[k] if wide == 2 else inv_ref[k]
        q_ref[tile, span(k, k + wide)] = dot_nt(x_ref[tile, span(k, k + wide)], factor)

    def project(first, last, tile):
        x_ref[tile, last * BLOCK:] = x_ref[tile, last * BLOCK:] - dot(
            q_ref[tile, span(first, last)], a_ref[span(first, last), last * BLOCK:]
        )

    def send(first, last):
        for b in range(first, last):
            stores[b].start()

    def solve_rows(k, p, work):
        rows = slice(k * BLOCK + p * PANEL, k * BLOCK + (p + 1) * PANEL)
        lane = lax.broadcasted_iota(jnp.int32, (PANEL, BLOCK), 1)
        left = jnp.where(lane < (p + 1) * PANEL, work[p * PANEL:(p + 1) * PANEL, :], 0.0)
        value = dot(left, original[...])
        a_ref[rows, span(k + 1, k + 2)] = value
        return value

    def after(k):
        first = k // 2 * 2
        if k + 1 == NBLK:
            return
        if k % 2 == 0:
            soon.append(lambda: couple(k))
            if k + 2 < NBLK:
                soon.append(lambda: solve(k, k + 2))
                soon.append(lambda: downdate(k + 1, k + 2, k, k + 1))
                soon.append(lambda: downdate(k + 2, k + 2, k, k + 1))
            if k + 3 < NBLK:
                soon.append(lambda: solve(k, k + 3, NBLK - k - 3))
                soon.append(lambda: downdate(k + 1, k + 3, k, k + 1, NBLK - k - 3))
        else:
            if k + 2 < NBLK:
                soon.append(lambda: solve(k, k + 2, NBLK - k - 2))
                soon.append(lambda: downdate(k + 1, k + 2, first, k + 1, NBLK - k - 2))
                for i in range(k + 2, NBLK):
                    soon.append(lambda i=i: downdate(i, i, first, k + 1, NBLK - i))
            whenever.append(lambda: pair(first))
            for tile in tiles:
                whenever.append(lambda tile=tile: finish(first, 2, tile))
            whenever.append(lambda: send(first, k + 1))
            for tile in tiles:
                whenever.append(lambda tile=tile: project(first, k + 1, tile))

    def run(queue, count):
        for _ in range(min(count, len(queue))):
            queue.pop(0)()

    inv_ref[0] = jnp.where(lower, lead_ref[...], 0.0)
    solve(0, 1)
    turned = a(0, 1).T
    for first, last in ((0, PANEL), (PANEL, BLOCK)):
        work_ref[1, first:last, :] = a_ref[BLOCK + first:BLOCK + last, span(1, 2)] - dot(
            turned[first:last, :], a(0, 1)
        )
    after(0)
    for k in range(1, NBLK):
        work = work_ref.at[k % 2]
        following = work_ref.at[1 - k % 2]
        original = next_ref.at[k % 2]
        more = k + 1 < NBLK
        early = (PANELS - 1) * PANEL

        def after_panel(p):
            if p == PANELS - 1:
                return
            left = PANELS - 1 - p
            run(soon, -(-len(soon) // max(left - 1, 1)))
            if p == PANELS - 2:
                run(soon, len(soon))
                if more:
                    original[...] = a(k, k + 1)
                    for done in range(PANELS - 1):
                        solve_rows(k, done, work)
                    solved = a_ref[k * BLOCK:k * BLOCK + early, span(k + 1, k + 2)]
                    following[...] = a(k + 1, k + 1) - dot_tn(solved, solved)
            turns = left + (PANELS - 1 if k % 2 == 0 and more else 0)
            run(whenever, -(-len(whenever) // turns))

        eliminate(work, col_ref, row_ref, after_panel)
        if more:
            value = solve_rows(k, PANELS - 1, work)
            turned = value.T
            for first, last in ((0, PANEL), (PANEL, BLOCK)):
                following[first:last, :] = following[first:last, :] - dot(turned[first:last, :], value)
        inv_ref[k] = jnp.where(lower, work[...], 0.0)
        if k == 1:
            for load in loads:
                load.wait()
        after(k)
    run(whenever, len(whenever))
    for t, tile in enumerate(tiles):
        finish(final, 1, tile)
        stores[final + t].start()
    for store in stores:
        store.wait()


def vmem():
    return pl.BlockSpec(memory_space=pltpu.VMEM)


def smem():
    return pl.BlockSpec(memory_space=pltpu.SMEM)


def anywhere():
    return pl.BlockSpec(memory_space=pl.ANY)


def finish_scratch(rows):
    bands = NBLK * BLOCK
    return [
        pltpu.VMEM((bands, bands), jnp.float32),
        pltpu.VMEM((NBLK, BLOCK, BLOCK), jnp.float32),
        pltpu.VMEM((NBLK, 2 * BLOCK, 2 * BLOCK), jnp.float32),
        pltpu.VMEM((rows, bands), jnp.float32),
        pltpu.VMEM((rows, bands), jnp.float32),
        pltpu.VMEM((2, BLOCK, BLOCK), jnp.float32),
        pltpu.VMEM((2, BLOCK, BLOCK), jnp.float32),
        pltpu.VMEM((PANEL, PANEL, BLOCK), jnp.float32),
        pltpu.VMEM((PANEL, PANEL, BLOCK), jnp.float32),
        pltpu.SemaphoreType.DMA((NBLK,)),
        pltpu.SemaphoreType.DMA((NBLK - 1 + rows // BLOCK,)),
    ]


def local(psi, order):
    rows, bands = psi.shape
    size = lax.axis_size("grid")
    chips = size // 2
    scale = 1.0 / (rows * size)
    core = lax.axis_index("grid") % 2
    pairs = [(d, d ^ 1) for d in range(size)]
    groups = [list(range(c, size, 2)) for c in range(2)]
    half = SLOTS // 2
    chunk = half * BLOCK // chips

    core = core.astype(jnp.int32).reshape(1)
    shape = (half, BLOCK, BLOCK)
    send, x = pl.pallas_call(
        lambda *refs: send_kernel(scale, *refs),
        out_shape=[pltpu.VMEM(shape, jnp.float32), pltpu.VMEM((rows, bands), jnp.float32)],
        in_specs=[smem(), smem(), vmem()],
        out_specs=[vmem(), vmem()],
        name="gram_send",
    )(core, order, psi)
    x = pltpu.with_memory_space_constraint(x, pltpu.VMEM)
    keep = pl.pallas_call(
        lambda *refs: keep_kernel(scale, *refs),
        out_shape=pltpu.VMEM(shape, jnp.float32),
        in_specs=[smem(), vmem()],
        out_specs=vmem(),
        name="gram_keep",
    )(core, x)
    both = keep + lax.ppermute(send, "grid", pairs)
    parts = lax.all_to_all(
        both.reshape(chips, chunk, BLOCK), "grid", 0, 0, axis_index_groups=groups, tiled=True
    )
    total = jnp.sum(parts, axis=0)
    mine = lax.all_to_all(
        jnp.broadcast_to(total[None], parts.shape), "grid", 0, 0, axis_index_groups=groups, tiled=True
    ).reshape(half, BLOCK, BLOCK)
    other = lax.ppermute(mine, "grid", pairs)
    mine = pltpu.with_memory_space_constraint(mine, pltpu.VMEM)
    other = pltpu.with_memory_space_constraint(other, pltpu.VMEM)

    lead = pl.pallas_call(
        lead_kernel,
        out_shape=pltpu.VMEM((BLOCK, BLOCK), jnp.float32),
        in_specs=[smem(), vmem()],
        out_specs=vmem(),
        scratch_shapes=[
            pltpu.VMEM((BLOCK, BLOCK), jnp.float32),
            pltpu.VMEM((PANEL, PANEL, BLOCK), jnp.float32),
            pltpu.VMEM((PANEL, PANEL, BLOCK), jnp.float32),
        ],
        name="lead",
    )(core, mine)
    lead = pltpu.with_memory_space_constraint(lead, pltpu.VMEM)
    return pl.pallas_call(
        finish_kernel,
        out_shape=jax.ShapeDtypeStruct((rows, bands), jnp.float32),
        in_specs=[smem(), smem(), vmem(), vmem(), vmem(), anywhere()],
        out_specs=anywhere(),
        scratch_shapes=finish_scratch(rows),
        name="finish",
    )(core, order, lead, mine, other, psi)


def solution(mesh):
    in_specs = (P(("frag", "grid"), None), P("frag"))
    out_specs = P(("frag", "grid"), None)
    return jax.shard_map(local, mesh=mesh, in_specs=in_specs, out_specs=out_specs, check_vma=False)
```

```python
import jax
import jax.numpy as jnp
from jax import lax
from jax.experimental import pallas as pl
from jax.experimental.pallas import tpu as pltpu
from jax.sharding import PartitionSpec as P

BLOCK = 128
NBLK = 5
PANEL = 32
SUB = 8
PANELS = BLOCK // PANEL
PAIRS = [(i, j) for i in range(NBLK) for j in range(i, NBLK)]
SLOT = {pair: slot for slot, pair in enumerate(PAIRS)}
SLOTS = 16
LOADS = 4
HIGHEST = lax.Precision.HIGHEST


def dot(left, right):
    return lax.dot_general(
        left, right, (((1,), (0,)), ((), ())), precision=HIGHEST, preferred_element_type=jnp.float32
    )


def dot_tn(left, right):
    return lax.dot_general(
        left, right, (((0,), (0,)), ((), ())), precision=HIGHEST, preferred_element_type=jnp.float32
    )


def dot_nt(left, right):
    return lax.dot_general(
        left, right, (((1,), (1,)), ((), ())), precision=HIGHEST, preferred_element_type=jnp.float32
    )


def span(first, last):
    return slice(first * BLOCK, last * BLOCK)


def block_copies(order_ref, far_ref, near_ref, sems, count, outward=False):
    copies = []
    for b in range(count):
        start = pl.multiple_of(order_ref[b] * BLOCK, BLOCK)
        far = far_ref.at[:, pl.ds(start, BLOCK)]
        near = near_ref.at[:, span(b, b + 1)]
        copies.append(
            pltpu.make_async_copy(near, far, sems.at[b])
            if outward
            else pltpu.make_async_copy(far, near, sems.at[b])
        )
    return copies


def gram_half(scale, half, x_ref, out_ref):
    first = half * (SLOTS // 2)
    held = PAIRS[first:first + SLOTS // 2]
    for i in range(NBLK):
        js = [j for row, j in held if row == i]
        if js:
            row = dot_tn(x_ref[:, span(i, i + 1)], x_ref[:, span(js[0], js[-1] + 1)]) * scale
            for at, j in enumerate(js):
                out_ref[SLOT[i, j] - first] = row[:, span(at, at + 1)]
    if half == 1:
        lead = x_ref[:, span(0, 1)]
        out_ref[SLOTS // 2 - 1] = dot_tn(lead, lead) * scale


def send_kernel(scale, core_ref, order_ref, psi_ref, out_ref, x_ref, raw_ref, sems):
    rows = psi_ref.shape[0] // LOADS
    parts = [slice(t * rows, (t + 1) * rows) for t in range(LOADS)]
    loads = [
        pltpu.make_async_copy(psi_ref.at[part], raw_ref.at[part], sems.at[t])
        for t, part in enumerate(parts)
    ]
    for load in loads:
        load.start()
    starts = [pl.multiple_of(order_ref[i] * BLOCK, BLOCK) for i in range(NBLK)]
    for part, load in zip(parts, loads):
        load.wait()
        for i, start in enumerate(starts):
            x_ref[part, span(i, i + 1)] = raw_ref[part, pl.ds(start, BLOCK)]
    for core in range(2):
        pl.when(core_ref[0] == core)(lambda: gram_half(scale, 1 - core, x_ref, out_ref))


def keep_kernel(scale, core_ref, x_ref, out_ref):
    for core in range(2):
        pl.when(core_ref[0] == core)(lambda: gram_half(scale, core, x_ref, out_ref))


def eliminate(work_ref, col_ref, row_ref, after_panel):
    lane = lax.broadcasted_iota(jnp.int32, (SUB, BLOCK), 1)
    row = lax.broadcasted_iota(jnp.int32, (SUB, BLOCK), 0)
    pieces = PANEL // SUB
    for p in range(PANELS):
        r0 = p * PANEL
        low = r0 + PANEL
        for m in range(PANEL):
            top = m // SUB * SUB
            col_ref[m, top:, :] = jnp.broadcast_to(
                work_ref[r0 + top:low, r0 + m:r0 + m + 1], (PANEL - top, BLOCK)
            )
        inside = (lane >= r0) & (lane < low)
        part = []
        for q in range(pieces):
            unit = (lane == row + (r0 + q * SUB)).astype(jnp.float32)
            part.append(jnp.where(inside, unit, work_ref[r0 + q * SUB:r0 + (q + 1) * SUB, :]))
        diag = [jnp.ones((SUB, BLOCK), jnp.float32)] * pieces
        factors = {}
        for group in range(pieces):
            column = {}
            for m in range(group * SUB, (group + 1) * SUB):
                for q in range(group, pieces):
                    value = col_ref[m, q * SUB:(q + 1) * SUB, :]
                    for k in range(group * SUB):
                        value = value - factors[k, q] * row_ref[k, m:m + 1, :]
                    column[m, q] = value
            for k in range(group * SUB, (group + 1) * SUB):
                ks = k % SUB
                pivot = column[k, group][ks:ks + 1, :]
                inverse = 1.0 / pivot
                diag[group] = jnp.where(row == ks, pivot, diag[group])
                for q in range(group, pieces):
                    factors[k, q] = column[k, q] * inverse
                for q in range(group + 1, pieces):
                    row_ref[k, q * SUB:(q + 1) * SUB, :] = column[k, q]
                for m in range(k + 1, (group + 1) * SUB):
                    entry = column[k, group][m % SUB:m % SUB + 1, :]
                    for q in range(group, pieces):
                        column[m, q] = column[m, q] - factors[k, q] * entry
                lead = part[group][ks:ks + 1, :]
                part[group] = part[group] - jnp.where(row > ks, factors[k, group], 0.0) * lead
                for q in range(group + 1, pieces):
                    part[q] = part[q] - factors[k, q] * lead
        work_ref[r0:low, :] = jnp.concatenate(
            [part[q] * lax.rsqrt(diag[q]) for q in range(pieces)], axis=0
        )
        if low < BLOCK:
            turned = jnp.concatenate(part, axis=0).T
            scaled = jnp.concatenate([part[q] * (1.0 / diag[q]) for q in range(pieces)], axis=0)
            for first, last in ((low, low + PANEL), (low + PANEL, BLOCK)):
                if first < last:
                    rest = lax.broadcasted_iota(jnp.int32, (last - first, BLOCK), 1)
                    kept = jnp.where((rest >= r0) & (rest < low), 0.0, work_ref[first:last, :])
                    work_ref[first:last, :] = kept - dot(turned[first:last, :], scaled)
        after_panel(p)


def lead_kernel(core_ref, mine_ref, out_ref, work_ref, col_ref, row_ref):
    work_ref[...] = jnp.where(core_ref[0] == 0, mine_ref[0], mine_ref[SLOTS // 2 - 1])
    eliminate(work_ref, col_ref, row_ref, lambda p: None)
    out_ref[...] = work_ref[...]


def finish_kernel(
    core_ref, order_ref, lead_ref, mine_ref, other_ref, psi_ref, out_ref,
    a_ref, inv_ref, pair_ref, x_ref, q_ref, work_ref, next_ref, col_ref, row_ref, in_sems, out_sems,
):
    loads = block_copies(order_ref, psi_ref, x_ref, in_sems, NBLK)
    final = NBLK - 1
    stores = block_copies(order_ref, out_ref, q_ref, out_sems, final, outward=True)
    for load in loads:
        load.start()
    core = core_ref[0]
    half = SLOTS // 2
    for slot, (i, j) in enumerate(PAIRS):
        own = core == slot // half
        a_ref[span(i, i + 1), span(j, j + 1)] = jnp.where(
            own, mine_ref[slot % half], other_ref[slot % half]
        )
    lower = (
        lax.broadcasted_iota(jnp.int32, (BLOCK, BLOCK), 0)
        >= lax.broadcasted_iota(jnp.int32, (BLOCK, BLOCK), 1)
    )
    rows = x_ref.shape[0]
    tiles = [slice(r, r + BLOCK) for r in range(0, rows, BLOCK)]
    soon, whenever = [], []
    where_to = pl.multiple_of(order_ref[final] * BLOCK, BLOCK)
    stores = stores + [
        pltpu.make_async_copy(
            q_ref.at[tile, span(final, NBLK)],
            out_ref.at[tile, pl.ds(where_to, BLOCK)],
            out_sems.at[final + t],
        )
        for t, tile in enumerate(tiles)
    ]

    def a(i, j, wide=1):
        return a_ref[span(i, i + 1), span(j, j + wide)]

    def solve(k, j, wide=1):
        a_ref[span(k, k + 1), span(j, j + wide)] = dot(inv_ref[k], a(k, j, wide))

    def downdate(i, j, first, last, wide=1):
        ks = span(first, last)
        a_ref[span(i, i + 1), span(j, j + wide)] = a(i, j, wide) - dot_tn(
            a_ref[ks, span(i, i + 1)], a_ref[ks, span(j, j + wide)]
        )

    def couple(k):
        pair_ref[k, BLOCK:, :BLOCK] = dot_tn(a(k, k + 1), inv_ref[k])

    def pair(k):
        pair_ref[k, :BLOCK, :BLOCK] = inv_ref[k]
        pair_ref[k, BLOCK:, BLOCK:] = inv_ref[k + 1]
        pair_ref[k, :BLOCK, BLOCK:] = jnp.zeros((BLOCK, BLOCK), jnp.float32)
        pair_ref[k, BLOCK:, :BLOCK] = -dot(inv_ref[k + 1], pair_ref[k, BLOCK:, :BLOCK])

    def finish(k, wide, tile):
        factor = pair_ref[k] if wide == 2 else inv_ref[k]
        q_ref[tile, span(k, k + wide)] = dot_nt(x_ref[tile, span(k, k + wide)], factor)

    def project(first, last, tile):
        x_ref[tile, last * BLOCK:] = x_ref[tile, last * BLOCK:] - dot(
            q_ref[tile, span(first, last)], a_ref[span(first, last), last * BLOCK:]
        )

    def send(first, last):
        for b in range(first, last):
            stores[b].start()

    def solve_rows(k, p, work):
        rows = slice(k * BLOCK + p * PANEL, k * BLOCK + (p + 1) * PANEL)
        lane = lax.broadcasted_iota(jnp.int32, (PANEL, BLOCK), 1)
        left = jnp.where(lane < (p + 1) * PANEL, work[p * PANEL:(p + 1) * PANEL, :], 0.0)
        value = dot(left, original[...])
        a_ref[rows, span(k + 1, k + 2)] = value
        return value

    def after(k):
        first = k // 2 * 2
        if k + 1 == NBLK:
            return
        if k % 2 == 0:
            soon.append(lambda: couple(k))
            if k + 2 < NBLK:
                soon.append(lambda: solve(k, k + 2))
                soon.append(lambda: downdate(k + 1, k + 2, k, k + 1))
                soon.append(lambda: downdate(k + 2, k + 2, k, k + 1))
            if k + 3 < NBLK:
                soon.append(lambda: solve(k, k + 3, NBLK - k - 3))
                soon.append(lambda: downdate(k + 1, k + 3, k, k + 1, NBLK - k - 3))
        else:
            if k + 2 < NBLK:
                soon.append(lambda: solve(k, k + 2, NBLK - k - 2))
                soon.append(lambda: downdate(k + 1, k + 2, first, k + 1, NBLK - k - 2))
                for i in range(k + 2, NBLK):
                    soon.append(lambda i=i: downdate(i, i, first, k + 1, NBLK - i))
            whenever.append(lambda: pair(first))
            for tile in tiles:
                whenever.append(lambda tile=tile: finish(first, 2, tile))
            whenever.append(lambda: send(first, k + 1))
            for tile in tiles:
                whenever.append(lambda tile=tile: project(first, k + 1, tile))

    def run(queue, count):
        for _ in range(min(count, len(queue))):
            queue.pop(0)()

    inv_ref[0] = jnp.where(lower, lead_ref[...], 0.0)
    solve(0, 1)
    turned = a(0, 1).T
    for first, last in ((0, PANEL), (PANEL, BLOCK)):
        work_ref[1, first:last, :] = a_ref[BLOCK + first:BLOCK + last, span(1, 2)] - dot(
            turned[first:last, :], a(0, 1)
        )
    after(0)
    for k in range(1, NBLK):
        work = work_ref.at[k % 2]
        following = work_ref.at[1 - k % 2]
        original = next_ref.at[k % 2]
        more = k + 1 < NBLK
        early = (PANELS - 1) * PANEL

        def after_panel(p):
            if p == PANELS - 1:
                return
            left = PANELS - 1 - p
            run(soon, -(-len(soon) // max(left - 1, 1)))
            if p == PANELS - 2:
                run(soon, len(soon))
                if more:
                    original[...] = a(k, k + 1)
                    for done in range(PANELS - 1):
                        solve_rows(k, done, work)
                    solved = a_ref[k * BLOCK:k * BLOCK + early, span(k + 1, k + 2)]
                    following[...] = a(k + 1, k + 1) - dot_tn(solved, solved)
            turns = left + (PANELS - 1 if k % 2 == 0 and more else 0)
            run(whenever, -(-len(whenever) // turns))

        eliminate(work, col_ref, row_ref, after_panel)
        if more:
            value = solve_rows(k, PANELS - 1, work)
            turned = value.T
            for first, last in ((0, PANEL), (PANEL, BLOCK)):
                following[first:last, :] = following[first:last, :] - dot(turned[first:last, :], value)
        inv_ref[k] = jnp.where(lower, work[...], 0.0)
        if k == 1:
            for load in loads:
                load.wait()
        after(k)
    run(whenever, len(whenever))
    for t, tile in enumerate(tiles):
        finish(final, 1, tile)
        stores[final + t].start()
    for store in stores:
        store.wait()


def vmem():
    return pl.BlockSpec(memory_space=pltpu.VMEM)


def smem():
    return pl.BlockSpec(memory_space=pltpu.SMEM)


def anywhere():
    return pl.BlockSpec(memory_space=pl.ANY)


def finish_scratch(rows):
    bands = NBLK * BLOCK
    return [
        pltpu.VMEM((bands, bands), jnp.float32),
        pltpu.VMEM((NBLK, BLOCK, BLOCK), jnp.float32),
        pltpu.VMEM((NBLK, 2 * BLOCK, 2 * BLOCK), jnp.float32),
        pltpu.VMEM((rows, bands), jnp.float32),
        pltpu.VMEM((rows, bands), jnp.float32),
        pltpu.VMEM((2, BLOCK, BLOCK), jnp.float32),
        pltpu.VMEM((2, BLOCK, BLOCK), jnp.float32),
        pltpu.VMEM((PANEL, PANEL, BLOCK), jnp.float32),
        pltpu.VMEM((PANEL, PANEL, BLOCK), jnp.float32),
        pltpu.SemaphoreType.DMA((NBLK,)),
        pltpu.SemaphoreType.DMA((NBLK - 1 + rows // BLOCK,)),
    ]


def local(psi, order):
    rows, bands = psi.shape
    size = lax.axis_size("grid")
    chips = size // 2
    scale = 1.0 / (rows * size)
    core = lax.axis_index("grid") % 2
    pairs = [(d, d ^ 1) for d in range(size)]
    groups = [list(range(c, size, 2)) for c in range(2)]
    half = SLOTS // 2
    chunk = half * BLOCK // chips

    core = core.astype(jnp.int32).reshape(1)
    shape = (half, BLOCK, BLOCK)
    send, x = pl.pallas_call(
        lambda *refs: send_kernel(scale, *refs),
        out_shape=[pltpu.VMEM(shape, jnp.float32), pltpu.VMEM((rows, bands), jnp.float32)],
        in_specs=[smem(), smem(), anywhere()],
        out_specs=[vmem(), vmem()],
        scratch_shapes=[
            pltpu.VMEM((rows, bands), jnp.float32),
            pltpu.SemaphoreType.DMA((LOADS,)),
        ],
        name="gram_send",
    )(core, order, psi)
    x = pltpu.with_memory_space_constraint(x, pltpu.VMEM)
    keep = pl.pallas_call(
        lambda *refs: keep_kernel(scale, *refs),
        out_shape=pltpu.VMEM(shape, jnp.float32),
        in_specs=[smem(), vmem()],
        out_specs=vmem(),
        name="gram_keep",
    )(core, x)
    both = keep + lax.ppermute(send, "grid", pairs)
    parts = lax.all_to_all(
        both.reshape(chips, chunk, BLOCK), "grid", 0, 0, axis_index_groups=groups, tiled=True
    )
    total = jnp.sum(parts, axis=0)
    mine = lax.all_to_all(
        jnp.broadcast_to(total[None], parts.shape), "grid", 0, 0, axis_index_groups=groups, tiled=True
    ).reshape(half, BLOCK, BLOCK)
    other = lax.ppermute(mine, "grid", pairs)
    mine = pltpu.with_memory_space_constraint(mine, pltpu.VMEM)
    other = pltpu.with_memory_space_constraint(other, pltpu.VMEM)

    lead = pl.pallas_call(
        lead_kernel,
        out_shape=pltpu.VMEM((BLOCK, BLOCK), jnp.float32),
        in_specs=[smem(), vmem()],
        out_specs=vmem(),
        scratch_shapes=[
            pltpu.VMEM((BLOCK, BLOCK), jnp.float32),
            pltpu.VMEM((PANEL, PANEL, BLOCK), jnp.float32),
            pltpu.VMEM((PANEL, PANEL, BLOCK), jnp.float32),
        ],
        name="lead",
    )(core, mine)
    lead = pltpu.with_memory_space_constraint(lead, pltpu.VMEM)
    return pl.pallas_call(
        finish_kernel,
        out_shape=jax.ShapeDtypeStruct((rows, bands), jnp.float32),
        in_specs=[smem(), smem(), vmem(), vmem(), vmem(), anywhere()],
        out_specs=anywhere(),
        scratch_shapes=finish_scratch(rows),
        name="finish",
    )(core, order, lead, mine, other, psi)


def solution(mesh):
    in_specs = (P(("frag", "grid"), None), P("frag"))
    out_specs = P(("frag", "grid"), None)
    return jax.shard_map(local, mesh=mesh, in_specs=in_specs, out_specs=out_specs, check_vma=False)
```
